128 devices in a mesh: dp: 4 (over x), vocab: 32 (over z, y, core).
Axes of the slice: x: 4, y: 4, z: 4, core: 2. Of those that a mesh axis runs over, the one named last changes fastest.
Arguments:
- token_ids: int32 [524288], P(('dp', 'vocab')), may hold values from 0 to 30719, as said below
- valid_counts: int32 [4096], P(('dp', 'vocab')), may hold values from 64 to 128
- grad_output: bfloat16 [524288, 768], P(('dp', 'vocab')), may hold values from -6 to 6
- pre_norm: bfloat16 [524288, 768], P(('dp', 'vocab')), may hold values from -6 to 6
- norm_gain: float32 [768], replicated, may hold values from 0.5 to 1.5
Outputs:
- grad_table: float32 [30720, 768], P('vocab')
The draws below stay inside these ranges and needn't reach their ends.
Inputs may be any that keep to these rules, and one draw needn't show every extreme that they name: `token_ids`: of the 4096 positions of one device, at most 256 have ids in any one range [k * 960, (k + 1) * 960); in every group of 32 consecutive devices one such range takes exactly 256 from every device of the group. Padding positions carry ids too.
All inputs are finite; a program needn't handle non-finite values.
Results may differ from the reference program's by a relative error of at most 0.0029.
Values may be sent and summed in bfloat16 or wider, within the bound.
A program may use at most 128 MiB of HBM per device.

```python
import jax
import jax.numpy as jnp
from jax import lax

D = 768
VOCAB_DEV = 960
BLOCK = 128
TOK_DEV = 4096
VOCAB = 30720
TOKENS = 524288
BLOCKS = 4096
CAP = 256
N_DP = 4
N_VOCAB = 32
DEVICES = 128


def draw_token_ids(key, part):
    keys = jax.random.split(key, 6)
    slots = N_VOCAB * CAP
    hottest = jax.random.randint(keys[0], (N_DP,), 0, N_VOCAB)
    hot_dev = jnp.repeat(hottest, N_VOCAB)
    prefer = jax.random.randint(keys[1], (DEVICES, N_VOCAB), 0, 4)
    noise = jax.random.randint(keys[2], (DEVICES, slots), 0, 4096)
    owner_of = jnp.arange(slots, dtype=jnp.int32) // CAP
    score = prefer[:, owner_of] * 4096 + noise
    score = jnp.where(owner_of[None, :] == hot_dev[:, None], -1, score)
    score = score * slots + jnp.arange(slots, dtype=jnp.int32)[None, :]
    chosen = jnp.argsort(score, axis=1, stable=True)[:, :TOK_DEV]
    owners = chosen // CAP
    owners = jax.random.permutation(keys[3], owners, axis=1, independent=True)
    first_term = jax.random.randint(keys[4], (DEVICES, TOK_DEV), 0, VOCAB_DEV)
    second_term = jax.random.randint(keys[5], (DEVICES, TOK_DEV), 0, VOCAB_DEV)
    offsets = jnp.minimum(first_term, second_term)
    return (owners * VOCAB_DEV + offsets).reshape(-1).astype(jnp.int32)


def plant(entries, stream_key, low, top_value):
    spot = [jax.random.randint(jax.random.fold_in(stream_key, axis), (), 0, length) for axis, length in enumerate(entries.shape)]
    widest = entries.shape.index(max(entries.shape))
    next_to = spot[:widest] + [(spot[widest] + 1) % entries.shape[widest]] + spot[widest + 1:]
    return entries.at[tuple(spot)].set(low).at[tuple(next_to)].set(top_value)


def steps_of(key, dims, cuts, smallest, high):
    level = 1.0
    for axis_at, blocks in cuts:
        draws = jax.random.uniform(jax.random.fold_in(jax.random.fold_in(key, 6), axis_at), (blocks,), jnp.float32, smallest / len(cuts), high / len(cuts))
        level = level * jnp.repeat(jnp.exp(draws), dims[axis_at] // blocks).reshape((-1,) + (1,) * (len(dims) - 1 - axis_at))
    return level


def normal_values(rng, dims, deviation, bound, shards=(), held_as=jnp.bfloat16):
    array = deviation * jax.random.normal(rng, dims, jnp.float32)
    if shards:
        array = array * steps_of(rng, dims, shards, -0.22, 0.18)
    return jnp.clip(array, -bound, bound).astype(held_as)


def setup_inputs(seed: int = 0) -> dict:
    arg_keys = jax.random.split(jax.random.key(seed), 6)
    return {
        "token_ids": draw_token_ids(jax.random.fold_in(arg_keys[5], 71), 0),
        "valid_counts": plant(jax.random.randint(arg_keys[1], (BLOCKS,), 64, BLOCK + 1), jax.random.fold_in(arg_keys[1], 1), 64, BLOCK).astype(jnp.int32),
        "grad_output": normal_values(arg_keys[2], (TOKENS, D), 1.0, 6.0, ((0, 128),)),
        "pre_norm": normal_values(arg_keys[3], (TOKENS, D), 1.0, 6.0, ((0, 128),)),
        "norm_gain": jnp.clip(1.0 + 0.1 * jax.random.normal(arg_keys[4], (D,), jnp.float32), 0.5, 1.5),
    }


def row_grads(grads, values, counts, gain):
    x = values.astype(jnp.float32)
    mu = lax.optimization_barrier(jnp.mean(x, axis=1, keepdims=True))
    centered_input = x - mu
    inverse_deviation = lax.rsqrt(lax.optimization_barrier(jnp.mean(centered_input * centered_input, axis=1, keepdims=True)) + 1e-12)
    normalized_input = centered_input * inverse_deviation
    scaled_gradient = gain[None, :] * grads.astype(jnp.float32)
    first_term = lax.optimization_barrier(jnp.mean(scaled_gradient, axis=1, keepdims=True))
    second_term = lax.optimization_barrier(jnp.mean(scaled_gradient * normalized_input, axis=1, keepdims=True))
    input_gradient = inverse_deviation * (scaled_gradient - first_term - normalized_input * second_term)
    place = jnp.arange(x.shape[0], dtype=jnp.int32) % BLOCK
    alive = place < jnp.repeat(counts, BLOCK)
    return jnp.where(alive[:, None], input_gradient, 0.0).astype(jnp.bfloat16)

def reference(token_ids, valid_counts, grad_output, pre_norm, norm_gain):
    ids = token_ids.reshape(DEVICES, TOK_DEV)
    counts = valid_counts.reshape(DEVICES, TOK_DEV // BLOCK)
    grads = grad_output.reshape(DEVICES, TOK_DEV, D)
    values = pre_norm.reshape(DEVICES, TOK_DEV, D)

    def step(table, item):
        ids_part, count_part, grad_part, value_part = item
        rows = row_grads(grad_part, value_part, count_part, norm_gain)
        table = table + jax.ops.segment_sum(rows.astype(jnp.float32), ids_part, num_segments=VOCAB)
        return (table, None)
    start = jnp.zeros((VOCAB, D), jnp.float32)
    table, _ = lax.scan(step, start, (ids, counts, grads, values))
    return table
```

```python
import functools

import jax
import jax.numpy as jnp
from jax import lax
from jax.experimental import pallas as pl
from jax.experimental.pallas import tpu as pltpu
from jax.sharding import PartitionSpec as P

VOCAB_DEV = 960
BLOCK = 128
CAP = 256
QROWS = VOCAB_DEV // 4
MESH = pl.DeviceIdType.MESH
F32, BF16, I32 = jnp.float32, jnp.bfloat16, jnp.int32


def place():
    x = lax.axis_index("dp")
    v = lax.axis_index("vocab")
    return x, v // 8, (v // 2) % 4, v % 2


def device(x, z, y, c):
    return (x, z * 8 + y * 2 + c)


def shifted(axis, d, dc=0):
    x, z, y, c = place()
    c = (c + dc) % 2
    if axis == "x":
        return device((x + d) % 4, z, y, c)
    if axis == "y":
        return device(x, z, (y + d) % 4, c)
    return device(x, (z + d) % 4, y, c)


def coordinate(axis):
    x, z, y, _ = place()
    return {"x": x, "y": y, "z": z}[axis]


def routing(token_ids, valid_counts):
    toks = token_ids.shape[0]
    blocks = toks // BLOCK
    owner = token_ids // VOCAB_DEV
    within = token_ids - owner * VOCAB_DEV
    place_in = jnp.arange(toks, dtype=I32) % BLOCK
    alive = (place_in.reshape(blocks, BLOCK) < valid_counts[:, None]).reshape(toks)
    marks = owner[:, None] == jnp.arange(32, dtype=I32)[None, :]
    marks3 = marks.astype(BF16).reshape(blocks, BLOCK, 32)
    tri = (jnp.arange(BLOCK)[:, None] > jnp.arange(BLOCK)[None, :]).astype(BF16)
    ahead = jnp.einsum("ij,bjk->bik", tri, marks3, preferred_element_type=F32)
    totals = jnp.sum(marks3.astype(F32), axis=1)
    tri_b = jnp.arange(blocks)[:, None] > jnp.arange(blocks)[None, :]
    base = jnp.sum(jnp.where(tri_b[:, :, None], totals[None], 0.0), axis=1)
    rank = jnp.sum(
        jnp.where(marks.reshape(blocks, BLOCK, 32), ahead + base[:, None, :], 0.0), axis=2
    )
    rank = rank.reshape(toks).astype(I32)
    fill = jnp.sum(totals, axis=0).astype(I32)
    target = owner * CAP + rank
    slot_marks = (rank[:, None] == jnp.arange(CAP, dtype=I32)[None, :]).astype(BF16)
    parts = jnp.stack([alive.astype(I32), within // 32, within % 32])
    parts = jnp.where(alive[None], parts, 0).astype(BF16)
    weights = parts[:, None, :] * marks.T.astype(BF16)[None]
    table = jnp.dot(
        weights.reshape(96, toks), slot_marks, preferred_element_type=F32
    ).reshape(3, 32, CAP)
    labels = jnp.where(table[0] > 0.5, table[1] * 32 + table[2], -1.0).astype(I32)
    return target, fill, labels


ROWS = 512


def dispatch_kernel(tgt, fill, counts, g_ref, v_ref, gain_ref, out_ref, rows, slots):
    step = pl.program_id(0)
    n_in = 4096 // ROWS
    plane = slots.shape[0] // 6

    @pl.when(step < n_in)
    def _():
        gain = gain_ref[...]
        for sub in range(ROWS // BLOCK):
            here = pl.ds(sub * BLOCK, BLOCK)
            x = v_ref[here, :].astype(F32)
            mu = jnp.mean(x, axis=1, keepdims=True)
            cen = x - mu
            inv = lax.rsqrt(jnp.mean(cen * cen, axis=1, keepdims=True) + 1e-12)
            scaled = gain * g_ref[here, :].astype(F32)
            first = jnp.mean(scaled, axis=1, keepdims=True)
            xhat = cen * inv
            second = jnp.mean(scaled * xhat, axis=1, keepdims=True)
            dx = inv * (scaled - first - xhat * second)
            live = lax.broadcasted_iota(I32, (BLOCK, 1), 0) < counts[step * (ROWS // BLOCK) + sub]
            dx = jnp.where(live, dx, 0.0)
            for j in range(6):
                rows[pl.ds(j * ROWS + sub * BLOCK, BLOCK), :] = dx[:, j * 128 : (j + 1) * 128]

        def body(i, carry):
            for u in range(8):
                t = tgt[step * ROWS + i * 8 + u]
                row = rows[pl.ds(i * 8 + u, 6, stride=ROWS), :]
                slots[pl.ds(t, 6, stride=plane), :] = row
            return carry

        lax.fori_loop(0, ROWS // 8, body, 0)

    @pl.when(step >= n_in)
    def _():
        at = step - n_in
        for k in range(4):
            filled = lax.broadcasted_iota(I32, (CAP, 1), 0) < fill[at * 4 + k]
            for j in range(6):
                part = slots[pl.ds(j * plane + (at * 4 + k) * CAP, CAP), :]
                out_ref[j // 2, pl.ds(k * CAP, CAP), pl.ds((j % 2) * 128, 128)] = jnp.where(
                    filled, part, 0.0
                ).astype(BF16)


def dispatch(target, fill, counts, grads, values, gain):
    n_in = 4096 // ROWS
    return pl.pallas_call(
        dispatch_kernel,
        out_shape=jax.ShapeDtypeStruct((3, 32 * CAP, 256), BF16),
        grid_spec=pltpu.PrefetchScalarGridSpec(
            num_scalar_prefetch=3,
            grid=(n_in + 8,),
            in_specs=[
                pl.BlockSpec((ROWS, 768), lambda i, *_: (jnp.minimum(i, n_in - 1), 0)),
                pl.BlockSpec((ROWS, 768), lambda i, *_: (jnp.minimum(i, n_in - 1), 0)),
                pl.BlockSpec((1, 768), lambda i, *_: (0, 0)),
            ],
            out_specs=pl.BlockSpec((3, 4 * CAP, 256), lambda i, *_: (0, jnp.maximum(i - n_in, 0), 0)),
            scratch_shapes=[
                pltpu.VMEM((6 * ROWS, 128), F32),
                pltpu.VMEM((6 * (32 * CAP + 8), 128), F32),
            ],
        ),
        compiler_params=pltpu.CompilerParams(vmem_limit_bytes=48 << 20),
        name="dispatch",
    )(target, fill, counts, grads, values, gain.reshape(1, 768))


ROW_AXES = ("z", "y", "x")


def exchange_kernel(box, lab, inbox, inlab, ss, rs, lss, lrs, own):
    x, z, y, c = place()
    barrier = pltpu.get_barrier_semaphore()
    hops = [(a, d, dc) for a in ROW_AXES for d in (1, 2, 3) for dc in (0, 1)] + [("x", 0, 1)]
    for a, d, dc in hops:
        pl.semaphore_signal(barrier, 1, device_id=shifted(a, d, dc), device_id_type=MESH)
    pl.semaphore_wait(barrier, len(hops))
    copies = []
    for d in (2, 1, 3, 0):
        for dc in (0, 1):
            for ch, a in enumerate(ROW_AXES):
                me = coordinate(a)
                q = (me + d) % 4
                cq = (c + dc) % 2
                for src, dst, s, r in ((box, inbox, ss, rs), (lab, inlab, lss, lrs)):
                    if src is box:
                        piece = box.at[ch, :, q, cq] if a == "y" else box.at[ch, q, :, cq]
                    else:
                        piece = lab.at[:, q, cq] if a == "y" else lab.at[q, :, cq]
                    if d == 0 and dc == 0:
                        copy = pltpu.make_async_copy(
                            piece, dst.at[ch, me, c], own.at[ch, 0 if src is box else 1]
                        )
                    else:
                        copy = pltpu.make_async_remote_copy(
                            src_ref=piece,
                            dst_ref=dst.at[ch, me, c],
                            send_sem=s.at[ch, d, dc],
                            recv_sem=r.at[ch, d, dc],
                            device_id=shifted(a, d, dc),
                            device_id_type=MESH,
                        )
                    copy.start()
                    copies.append(copy)
    for copy in copies:
        copy.wait()


def exchange(outbox, labels):
    any_space = pl.BlockSpec(memory_space=pl.ANY)
    return pl.pallas_call(
        exchange_kernel,
        out_shape=(
            jax.ShapeDtypeStruct((3, 4, 2, 4, CAP, 256), BF16),
            jax.ShapeDtypeStruct((3, 4, 2, 4, 2, 128), I32),
        ),
        in_specs=[any_space] * 2,
        out_specs=(any_space, any_space),
        scratch_shapes=[pltpu.SemaphoreType.DMA((3, 4, 2))] * 4 + [pltpu.SemaphoreType.DMA((3, 2))],
        compiler_params=pltpu.CompilerParams(collective_id=0, has_side_effects=True),
        name="exchange",
    )(outbox.reshape(3, 4, 4, 2, CAP, 256), labels.reshape(4, 4, 2, 2, 128))


def combine_kernel(in_ref, lab_ref, out_ref, picks):
    for s in range(8):
        for h in range(2):
            lab = lab_ref[0, s // 2, s % 2, 0, pl.ds(h, 1), :]
            hit = lax.broadcasted_iota(I32, (VOCAB_DEV, 128), 0) == lab
            picks[:, pl.ds(s * 256 + h * 128, 128)] = jnp.where(hit, 1.0, 0.0).astype(BF16)
    rows = in_ref[0, :, :, 0].reshape(2048, 256)
    for m in range(4):
        here = pl.ds(m * QROWS, QROWS)
        out_ref[0, 0, here, :] = jnp.dot(
            picks[here, :], rows, preferred_element_type=F32
        ).astype(BF16)


def combine(inbox, inlab):
    return pl.pallas_call(
        combine_kernel,
        grid=(3, 4),
        out_shape=jax.ShapeDtypeStruct((3, 4, VOCAB_DEV, 256), BF16),
        in_specs=[
            pl.BlockSpec((1, 4, 2, 1, CAP, 256), lambda i, k: (i, 0, 0, k, 0, 0)),
            pl.BlockSpec((1, 4, 2, 1, 2, 128), lambda i, k: (i, 0, 0, k, 0, 0)),
        ],
        out_specs=pl.BlockSpec((1, 1, VOCAB_DEV, 256), lambda i, k: (i, k, 0, 0)),
        scratch_shapes=[pltpu.VMEM((VOCAB_DEV, 2048), BF16)],
        name="combine",
    )(inbox, inlab)


def reduce_kernel(tab, out, got2a, got2, u, ub, got3, f, s2, r2, s3, r3, s4, r4, own):
    x, z, y, c = place()
    barrier = pltpu.get_barrier_semaphore()
    hops = [(a, d) for a in ("x", "y", "z") for d in (1, 2, 3)]
    for a, d in hops:
        pl.semaphore_signal(barrier, 1, device_id=shifted(a, d), device_id_type=MESH)
    for e in range(4):
        pl.semaphore_signal(
            barrier, 1, device_id=device((z + 0 * e), (e + 0 * z), y, c), device_id_type=MESH
        )
    pl.semaphore_wait(barrier, len(hops) + 4)

    first, second = ("x", "z", "y"), ("y", "x", "z")

    def send2(ch, d):
        q = (coordinate(first[ch]) + d) % 4
        if ch == 0:
            src, dst = tab.at[0, :, pl.ds(pl.multiple_of(q * QROWS, 16), QROWS)], got2a.at[d - 1]
        else:
            src, dst = tab.at[ch, q], got2.at[ch - 1, d - 1]
        return pltpu.make_async_remote_copy(
            src_ref=src, dst_ref=dst, send_sem=s2.at[ch, d - 1], recv_sem=r2.at[ch, d - 1],
            device_id=shifted(first[ch], d), device_id_type=MESH,
        )

    def send3(ch, d):
        q = (coordinate(second[ch]) + d) % 4
        return pltpu.make_async_remote_copy(
            src_ref=ub.at[ch, q], dst_ref=got3.at[ch, d - 1],
            send_sem=s3.at[ch, d - 1], recv_sem=r3.at[ch, d - 1],
            device_id=shifted(second[ch], d), device_id_type=MESH,
        )

    def send4(ch, d):
        dst = out.at[pl.ds(pl.multiple_of(x * QROWS, 16), QROWS), pl.ds(ch * 256, 256)]
        return pltpu.make_async_remote_copy(
            src_ref=f.at[ch], dst_ref=dst, send_sem=s4.at[ch, d], recv_sem=r4.at[ch, d],
            device_id=shifted("x", d), device_id_type=MESH,
        )

    twos = {(ch, d): send2(ch, d) for d in (2, 1, 3) for ch in range(3)}
    for copy in twos.values():
        copy.start()
    threes = {}
    for ch in range(3):
        for d in (1, 2, 3):
            twos[ch, d].wait()
        me = coordinate(first[ch])
        for p in range(4):
            at = pl.ds(p * QROWS, QROWS)
            if ch == 0:
                mine = tab[0, p, pl.ds(pl.multiple_of(me * QROWS, 16), QROWS), :].astype(F32)
                for d in range(3):
                    mine += got2a[d, p].astype(F32)
            else:
                mine = tab[ch, me, at, :].astype(F32)
                for d in range(3):
                    mine += got2[ch - 1, d, at, :].astype(F32)
            u[ch, p] = mine
            ub[ch, p] = mine.astype(BF16)
        for d in (2, 1, 3):
            threes[ch, d] = send3(ch, d)
            threes[ch, d].start()
    fours = []
    for ch in range(3):
        for d in (1, 2, 3):
            threes[ch, d].wait()
        me = coordinate(second[ch])
        total = u[ch, me]
        for d in range(3):
            total += got3[ch, d].astype(F32)
        f[ch] = total.astype(BF16)
        if ch < 2:
            out[pl.ds(pl.multiple_of(x * QROWS, 16), QROWS), pl.ds(ch * 256, 256)] = f[ch]
            for d in (2, 1, 3):
                copy = send4(ch, d)
                copy.start()
                fours.append(copy)
    rows = pl.ds(pl.multiple_of(z * QROWS, 16), QROWS)

    def send5(e):
        return pltpu.make_async_remote_copy(
            src_ref=f.at[2], dst_ref=out.at[rows, pl.ds(512, 256)],
            send_sem=s4.at[2, e], recv_sem=r4.at[2, z],
            device_id=device((x + e) % 4, x, y, c), device_id_type=MESH,
        )

    @pl.when(x == z)
    def _():
        out[rows, pl.ds(512, 256)] = f[2]

    for e in range(4):
        if e == 0:

            @pl.when(x != z)
            def _():
                send5(0).start()
        else:
            send5(e).start()
    for e in range(4):
        if e == 0:

            @pl.when(x != z)
            def _():
                send5(0).wait_send()
        else:
            send5(e).wait_send()
    for q in range(4):

        @pl.when(jnp.logical_or(x != z, q != z))
        def _():
            pltpu.make_async_remote_copy(
                src_ref=f.at[2], dst_ref=out.at[pl.ds(q * QROWS, QROWS), pl.ds(512, 256)],
                send_sem=s4.at[2, 0], recv_sem=r4.at[2, q],
                device_id=device(x, z, y, c), device_id_type=MESH,
            ).wait_recv()

    for copy in fours:
        copy.wait()


def reduce_tables(tables):
    vmem = pl.BlockSpec(memory_space=pltpu.VMEM)
    return pl.pallas_call(
        reduce_kernel,
        out_shape=jax.ShapeDtypeStruct((VOCAB_DEV, 768), BF16),
        in_specs=[vmem],
        out_specs=vmem,
        scratch_shapes=[
            pltpu.VMEM((3, 4, QROWS, 256), BF16),
            pltpu.VMEM((2, 3, VOCAB_DEV, 256), BF16),
            pltpu.VMEM((3, 4, QROWS, 256), F32),
            pltpu.VMEM((3, 4, QROWS, 256), BF16),
            pltpu.VMEM((3, 3, QROWS, 256), BF16),
            pltpu.VMEM((3, QROWS, 256), BF16),
            pltpu.SemaphoreType.DMA((3, 3)),
            pltpu.SemaphoreType.DMA((3, 3)),
            pltpu.SemaphoreType.DMA((3, 3)),
            pltpu.SemaphoreType.DMA((3, 3)),
            pltpu.SemaphoreType.DMA((3, 4)),
            pltpu.SemaphoreType.DMA((3, 4)),
            pltpu.SemaphoreType.DMA((1,)),
        ],
        compiler_params=pltpu.CompilerParams(collective_id=1, has_side_effects=True),
        name="reduce_tables",
    )(tables)


def per_device(token_ids, valid_counts, grad_output, pre_norm, norm_gain):
    target, fill, labels = routing(token_ids, valid_counts)
    outbox = dispatch(target, fill, valid_counts, grad_output, pre_norm, norm_gain)
    inbox, inlab = exchange(outbox, labels)
    tables = combine(inbox, inlab)
    return reduce_tables(tables).astype(F32)


def solution(mesh):
    in_specs = (
        P(("dp", "vocab")),
        P(("dp", "vocab")),
        P(("dp", "vocab"), None),
        P(("dp", "vocab"), None),
        P(),
    )
    return jax.shard_map(
        per_device, mesh=mesh, in_specs=in_specs, out_specs=P("vocab", None), check_vma=False
    )
```

```python
import functools

import jax
import jax.numpy as jnp
from jax import lax
from jax.experimental import pallas as pl
from jax.experimental.pallas import tpu as pltpu
from jax.sharding import PartitionSpec as P

VOCAB_DEV = 960
BLOCK = 128
CAP = 256
QROWS = VOCAB_DEV // 4
MESH = pl.DeviceIdType.MESH
F32, BF16, I32 = jnp.float32, jnp.bfloat16, jnp.int32


def place():
    x = lax.axis_index("dp")
    v = lax.axis_index("vocab")
    return x, v // 8, (v // 2) % 4, v % 2


def device(x, z, y, c):
    return (x, z * 8 + y * 2 + c)


def shifted(axis, d, dc=0):
    x, z, y, c = place()
    c = (c + dc) % 2
    if axis == "x":
        return device((x + d) % 4, z, y, c)
    if axis == "y":
        return device(x, z, (y + d) % 4, c)
    return device(x, (z + d) % 4, y, c)


def coordinate(axis):
    x, z, y, _ = place()
    return {"x": x, "y": y, "z": z}[axis]


def routing(token_ids, valid_counts):
    toks = token_ids.shape[0]
    blocks = toks // BLOCK
    owner = token_ids // VOCAB_DEV
    within = token_ids - owner * VOCAB_DEV
    place_in = jnp.arange(toks, dtype=I32) % BLOCK
    alive = (place_in.reshape(blocks, BLOCK) < valid_counts[:, None]).reshape(toks)
    marks = owner[:, None] == jnp.arange(32, dtype=I32)[None, :]
    marks3 = marks.astype(BF16).reshape(blocks, BLOCK, 32)
    tri = (jnp.arange(BLOCK)[:, None] > jnp.arange(BLOCK)[None, :]).astype(BF16)
    ahead = jnp.einsum("ij,bjk->bik", tri, marks3, preferred_element_type=F32)
    totals = jnp.sum(marks3.astype(F32), axis=1)
    tri_b = jnp.arange(blocks)[:, None] > jnp.arange(blocks)[None, :]
    base = jnp.sum(jnp.where(tri_b[:, :, None], totals[None], 0.0), axis=1)
    rank = jnp.sum(
        jnp.where(marks.reshape(blocks, BLOCK, 32), ahead + base[:, None, :], 0.0), axis=2
    )
    rank = rank.reshape(toks).astype(I32)
    fill = jnp.sum(totals, axis=0).astype(I32)
    target = owner * CAP + rank
    slot_marks = (rank[:, None] == jnp.arange(CAP, dtype=I32)[None, :]).astype(BF16)
    parts = jnp.stack([alive.astype(I32), within // 32, within % 32])
    parts = jnp.where(alive[None], parts, 0).astype(BF16)
    weights = parts[:, None, :] * marks.T.astype(BF16)[None]
    table = jnp.dot(
        weights.reshape(96, toks), slot_marks, preferred_element_type=F32
    ).reshape(3, 32, CAP)
    labels = jnp.where(table[0] > 0.5, table[1] * 32 + table[2], -1.0).astype(I32)
    return target, fill, labels


ROWS = 512


def dispatch_kernel(tgt, fill, counts, g_ref, v_ref, gain_ref, out_ref, rows, slots):
    step = pl.program_id(0)
    n_in = 4096 // ROWS
    plane = slots.shape[0] // 6

    @pl.when(step < n_in)
    def _():
        gain = gain_ref[...]
        for sub in range(ROWS // BLOCK):
            here = pl.ds(sub * BLOCK, BLOCK)
            x = v_ref[here, :].astype(F32)
            mu = jnp.mean(x, axis=1, keepdims=True)
            cen = x - mu
            inv = lax.rsqrt(jnp.mean(cen * cen, axis=1, keepdims=True) + 1e-12)
            scaled = gain * g_ref[here, :].astype(F32)
            first = jnp.mean(scaled, axis=1, keepdims=True)
            xhat = cen * inv
            second = jnp.mean(scaled * xhat, axis=1, keepdims=True)
            dx = inv * (scaled - first - xhat * second)
            live = lax.broadcasted_iota(I32, (BLOCK, 1), 0) < counts[step * (ROWS // BLOCK) + sub]
            dx = jnp.where(live, dx, 0.0)
            for j in range(6):
                rows[pl.ds(j * (ROWS + 8) + sub * BLOCK, BLOCK), :] = dx[:, j * 128 : (j + 1) * 128]

        def body(i, carry):
            for u in range(16):
                t = tgt[step * ROWS + i * 16 + u]
                row = rows[pl.ds(i * 16 + u, 6, stride=ROWS + 8), :]
                slots[pl.ds(t, 6, stride=plane), :] = row
            return carry

        lax.fori_loop(0, ROWS // 16, body, 0)

    @pl.when(step >= n_in)
    def _():
        at = step - n_in
        for k in range(4):
            filled = lax.broadcasted_iota(I32, (CAP, 1), 0) < fill[at * 4 + k]
            for j in range(6):
                part = slots[pl.ds(j * plane + (at * 4 + k) * CAP, CAP), :]
                out_ref[j // 2, pl.ds(k * CAP, CAP), pl.ds((j % 2) * 128, 128)] = jnp.where(
                    filled, part, 0.0
                ).astype(BF16)


def dispatch(target, fill, counts, grads, values, gain):
    n_in = 4096 // ROWS
    return pl.pallas_call(
        dispatch_kernel,
        out_shape=jax.ShapeDtypeStruct((3, 32 * CAP, 256), BF16),
        grid_spec=pltpu.PrefetchScalarGridSpec(
            num_scalar_prefetch=3,
            grid=(n_in + 8,),
            in_specs=[
                pl.BlockSpec((ROWS, 768), lambda i, *_: (jnp.minimum(i, n_in - 1), 0)),
                pl.BlockSpec((ROWS, 768), lambda i, *_: (jnp.minimum(i, n_in - 1), 0)),
                pl.BlockSpec((1, 768), lambda i, *_: (0, 0)),
            ],
            out_specs=pl.BlockSpec((3, 4 * CAP, 256), lambda i, *_: (0, jnp.maximum(i - n_in, 0), 0)),
            scratch_shapes=[
                pltpu.VMEM((6 * (ROWS + 8), 128), F32),
                pltpu.VMEM((6 * (32 * CAP + 8), 128), F32),
            ],
        ),
        compiler_params=pltpu.CompilerParams(vmem_limit_bytes=48 << 20),
        name="dispatch",
    )(target, fill, counts, grads, values, gain.reshape(1, 768))


ROW_AXES = ("z", "y", "x")
FIRST = ("x", "z", "y")
SECOND = ("y", "x", "z")
STEPS = (2, 1, 3, 0)


def quarter(ref, q):
    return ref.at[pl.ds(pl.multiple_of(q * QROWS, 16), QROWS)]


def table_kernel(
    box, lab, out, inbox, inlab, tab, got2a, got2, u0, u1, ub0, ub1, got3, f,
    s1, r1, sl, rl, own1, s2a, r2a, s2, r2, s3, r3, s4, r4,
):
    x, z, y, c = place()
    barrier = pltpu.get_barrier_semaphore()
    hops = [(a, d, dc) for a in ROW_AXES for d in (1, 2, 3) for dc in (0, 1)] + [("x", 0, 1)]
    for a, d, dc in hops:
        pl.semaphore_signal(barrier, 1, device_id=shifted(a, d, dc), device_id_type=MESH)
    for e in range(4):
        pl.semaphore_signal(barrier, 1, device_id=device(z, e, y, c), device_id_type=MESH)
    pl.semaphore_wait(barrier, len(hops) + 4)

    def remote(src, dst, send, recv, to):
        return pltpu.make_async_remote_copy(
            src_ref=src, dst_ref=dst, send_sem=send, recv_sem=recv, device_id=to, device_id_type=MESH
        )

    def owner_of(ch, r):
        return ((z if ch == 1 else y) + r) % 4

    def row_copy(ch, r, d, dc):
        q = (coordinate(ROW_AXES[ch]) + d) % 4
        w = owner_of(ch, r)
        cq = (c + dc) % 2
        src = box.at[ch, w, q, cq] if ch == 1 else box.at[ch, q, w, cq]
        k = d * 2 + dc
        if k == 0:
            return pltpu.make_async_copy(src, inbox.at[ch, r, 0], own1.at[ch, r])
        return remote(
            src, inbox.at[ch, r, k], s1.at[ch, r, k], r1.at[ch, r, k], shifted(ROW_AXES[ch], d, dc)
        )

    def label_copy(ch, d, dc):
        q = (coordinate(ROW_AXES[ch]) + d) % 4
        cq = (c + dc) % 2
        src = lab.at[:, q, cq] if ch == 1 else lab.at[q, :, cq]
        k = d * 2 + dc
        if k == 0:
            return pltpu.make_async_copy(src, inlab.at[ch, 0], own1.at[ch, 4])
        return remote(src, inlab.at[ch, k], sl.at[ch, k], rl.at[ch, k], shifted(ROW_AXES[ch], d, dc))

    routes = [(d, dc) for d in (2, 1, 3, 0) for dc in (0, 1)]
    labels = {}
    rows = {}
    for d, dc in routes:
        for ch in range(3):
            labels[ch, d, dc] = label_copy(ch, d, dc)
            labels[ch, d, dc].start()
    for r in STEPS:
        for d, dc in routes:
            for ch in range(3):
                rows[ch, r, d, dc] = row_copy(ch, r, d, dc)
                rows[ch, r, d, dc].start()

    def arrived(copy, local):
        if local:
            copy.wait()
        else:
            copy.wait_recv()

    twos = {}
    for r in STEPS:
        for ch in range(3):
            for d, dc in routes:
                if r == STEPS[0]:
                    arrived(labels[ch, d, dc], d + dc == 0)
                arrived(rows[ch, r, d, dc], d + dc == 0)
            w = owner_of(ch, r)

            def part(m, carry):
                ids = lax.broadcasted_iota(I32, (QROWS, 128), 0) + m * QROWS
                total = None
                for k in range(8):
                    picks = jnp.concatenate(
                        [
                            jnp.where(ids == inlab[ch, k, w, pl.ds(h, 1), :], 1.0, 0.0).astype(BF16)
                            for h in range(2)
                        ],
                        axis=1,
                    )
                    add = jnp.dot(picks, inbox[ch, r, k], preferred_element_type=F32)
                    total = add if total is None else total + add
                at = pl.ds(pl.multiple_of(m * QROWS, 16), QROWS)
                if ch > 0 and r == 0:
                    u1[ch - 1, at, :] = total
                else:
                    tab[ch, r, at, :] = total.astype(BF16)
                if ch == 0:

                    @pl.when(m == x)
                    def _():
                        u0[r] = total

                return carry

            lax.fori_loop(0, 4, part, 0)
            if ch == 0:
                for d in (2, 1, 3):
                    twos[0, r, d] = remote(
                        quarter(tab.at[0, r], (x + d) % 4), got2a.at[r, d - 1],
                        s2a.at[r, d - 1], r2a.at[r, d - 1], shifted("x", d),
                    )
                    twos[0, r, d].start()
            elif r > 0:
                twos[ch, r] = remote(
                    tab.at[ch, r], got2.at[ch - 1, r - 1],
                    s2.at[ch - 1, r - 1], r2.at[ch - 1, r - 1], shifted(FIRST[ch], r),
                )
                twos[ch, r].start()

    threes = {}
    for r in STEPS:
        for d in (2, 1, 3):
            twos[0, r, d].wait_recv()
        total = u0[r]
        for d in range(3):
            total += got2a[r, d].astype(F32)
        if r == 0:
            u0[0] = total
        else:
            ub0[r - 1] = total.astype(BF16)
            threes[0, r] = remote(
                ub0.at[r - 1], got3.at[0, r - 1], s3.at[0, r - 1], r3.at[0, r - 1], shifted("y", r)
            )
            threes[0, r].start()
    for ch in (1, 2):
        for r in (2, 1, 3):
            twos[ch, r].wait_recv()
        me = coordinate(SECOND[ch])
        for d in (2, 1, 3, 0):
            at = pl.ds(pl.multiple_of((me + d) % 4 * QROWS, 16), QROWS)
            total = u1[ch - 1, at, :]
            for e in range(3):
                total += got2[ch - 1, e, at, :].astype(F32)
            if d == 0:
                u1[ch - 1, at, :] = total
            else:
                ub1[ch - 1, d - 1] = total.astype(BF16)
                threes[ch, d] = remote(
                    ub1.at[ch - 1, d - 1], got3.at[ch, d - 1],
                    s3.at[ch, d - 1], r3.at[ch, d - 1], shifted(SECOND[ch], d),
                )
                threes[ch, d].start()

    fours = []
    for ch in range(3):
        for d in (2, 1, 3):
            threes[ch, d].wait_recv()
        if ch == 0:
            total = u0[0]
        else:
            me = coordinate(SECOND[ch])
            total = u1[ch - 1, pl.ds(pl.multiple_of(me * QROWS, 16), QROWS), :]
        for d in range(3):
            total += got3[ch, d].astype(F32)
        f[ch] = total.astype(BF16)
        if ch < 2:
            mine = out.at[pl.ds(pl.multiple_of(x * QROWS, 16), QROWS), pl.ds(ch * 256, 256)]
            mine[...] = f[ch]
            for d in (2, 1, 3):
                copy = remote(f.at[ch], mine, s4.at[ch, d], r4.at[ch, d], shifted("x", d))
                copy.start()
                fours.append(copy)

    mine = out.at[pl.ds(pl.multiple_of(z * QROWS, 16), QROWS), pl.ds(512, 256)]

    def last(e):
        return remote(f.at[2], mine, s4.at[2, e], r4.at[2, z], device((x + e) % 4, x, y, c))

    @pl.when(x == z)
    def _():
        mine[...] = f[2]

    @pl.when(x != z)
    def _():
        last(0).start()

    for e in (2, 1, 3):
        last(e).start()
    for q in range(4):

        @pl.when(jnp.logical_or(x != z, q != z))
        def _():
            remote(
                f.at[2], out.at[pl.ds(q * QROWS, QROWS), pl.ds(512, 256)],
                s4.at[2, 0], r4.at[2, q], device(x, z, y, c),
            ).wait_recv()

    for copy in fours:
        copy.wait()

    @pl.when(x != z)
    def _():
        last(0).wait_send()

    for e in (2, 1, 3):
        last(e).wait_send()
    for ch, d, dc in labels:
        if d + dc:
            labels[ch, d, dc].wait_send()
    for ch, r, d, dc in rows:
        if d + dc:
            rows[ch, r, d, dc].wait_send()
    for copy in list(twos.values()) + list(threes.values()):
        copy.wait_send()


def table_sums(outbox, labels):
    any_space = pl.BlockSpec(memory_space=pl.ANY)
    dma = pltpu.SemaphoreType.DMA
    return pl.pallas_call(
        table_kernel,
        out_shape=jax.ShapeDtypeStruct((VOCAB_DEV, 768), BF16),
        in_specs=[any_space] * 2,
        out_specs=pl.BlockSpec(memory_space=pltpu.VMEM),
        scratch_shapes=[
            pltpu.VMEM((3, 4, 8, CAP, 256), BF16),
            pltpu.VMEM((3, 8, 4, 2, 128), I32),
            pltpu.VMEM((3, 4, VOCAB_DEV, 256), BF16),
            pltpu.VMEM((4, 3, QROWS, 256), BF16),
            pltpu.VMEM((2, 3, VOCAB_DEV, 256), BF16),
            pltpu.VMEM((4, QROWS, 256), F32),
            pltpu.VMEM((2, VOCAB_DEV, 256), F32),
            pltpu.VMEM((3, QROWS, 256), BF16),
            pltpu.VMEM((2, 3, QROWS, 256), BF16),
            pltpu.VMEM((3, 3, QROWS, 256), BF16),
            pltpu.VMEM((3, QROWS, 256), BF16),
            dma((3, 4, 8)),
            dma((3, 4, 8)),
            dma((3, 8)),
            dma((3, 8)),
            dma((3, 5)),
            dma((4, 3)),
            dma((4, 3)),
            dma((2, 3)),
            dma((2, 3)),
            dma((3, 3)),
            dma((3, 3)),
            dma((3, 4)),
            dma((3, 4)),
        ],
        compiler_params=pltpu.CompilerParams(
            collective_id=0, has_side_effects=True, vmem_limit_bytes=56 << 20
        ),
        name="table_sums",
    )(outbox.reshape(3, 4, 4, 2, CAP, 256), labels.reshape(4, 4, 2, 2, 128))


def per_device(token_ids, valid_counts, grad_output, pre_norm, norm_gain):
    target, fill, labels = routing(token_ids, valid_counts)
    outbox = dispatch(target, fill, valid_counts, grad_output, pre_norm, norm_gain)
    return table_sums(outbox, labels).astype(F32)


def solution(mesh):
    in_specs = (
        P(("dp", "vocab")),
        P(("dp", "vocab")),
        P(("dp", "vocab"), None),
        P(("dp", "vocab"), None),
        P(),
    )
    return jax.shard_map(
        per_device, mesh=mesh, in_specs=in_specs, out_specs=P("vocab", None), check_vma=False
    )
```

```python
import functools

import jax
import jax.numpy as jnp
from jax import lax
from jax.experimental import pallas as pl
from jax.experimental.pallas import tpu as pltpu
from jax.sharding import PartitionSpec as P

VOCAB_DEV = 960
BLOCK = 128
CAP = 256
QROWS = VOCAB_DEV // 4
MESH = pl.DeviceIdType.MESH
F32, BF16, I32 = jnp.float32, jnp.bfloat16, jnp.int32


def place():
    x = lax.axis_index("dp")
    v = lax.axis_index("vocab")
    return x, v // 8, (v // 2) % 4, v % 2


def device(x, z, y, c):
    return (x, z * 8 + y * 2 + c)


def shifted(axis, d, dc=0):
    x, z, y, c = place()
    c = (c + dc) % 2
    if axis == "x":
        return device((x + d) % 4, z, y, c)
    if axis == "y":
        return device(x, z, (y + d) % 4, c)
    return device(x, (z + d) % 4, y, c)


def coordinate(axis):
    x, z, y, _ = place()
    return {"x": x, "y": y, "z": z}[axis]


TOKS = 4096
BLOCKS = TOKS // BLOCK


def routing_kernel(counts, ids_ref, tok_ref, lab_ref, weights, slots):
    owner_row = lax.broadcasted_iota(I32, (32, BLOCK), 0)
    lane = lax.broadcasted_iota(I32, (1, BLOCK), 1)
    ids = ids_ref[...]
    owner = lax.shift_right_logical(ids * 34953, 25)
    within = ids - owner * VOCAB_DEV
    before = (
        lax.broadcasted_iota(I32, (BLOCK, BLOCK), 0) < lax.broadcasted_iota(I32, (BLOCK, BLOCK), 1)
    )
    before = jnp.where(before, 1.0, 0.0).astype(BF16)
    base = jnp.zeros((32, 1), F32)
    slot_row = lax.broadcasted_iota(I32, (CAP, BLOCK), 0)
    for b in range(BLOCKS):
        mark = owner_row == owner[b : b + 1]
        ones = jnp.where(mark, 1.0, 0.0)
        ahead = jnp.dot(ones.astype(BF16), before, preferred_element_type=F32)
        rank = jnp.sum(jnp.where(mark, ahead + base, 0.0), axis=0, keepdims=True).astype(I32)
        base = base + jnp.sum(ones, axis=1, keepdims=True)
        live = lane < counts[b]
        mark = jnp.logical_and(mark, live)
        off = within[b : b + 1]
        at = pl.ds(b * BLOCK, BLOCK)
        for p, value in enumerate(
            (
                jnp.ones((1, BLOCK), F32),
                lax.shift_right_logical(off, 5).astype(F32),
                (off & 31).astype(F32),
                (b * 2 + lax.shift_right_logical(lane, 6)).astype(F32),
                (lane & 63).astype(F32),
            )
        ):
            weights[pl.ds(p * 32, 32), at] = jnp.where(mark, value, 0.0).astype(BF16)
        slots[:, at] = jnp.where(slot_row == rank, 1.0, 0.0).astype(BF16)
    table = lax.dot_general(
        weights[...], slots[...], (((1,), (1,)), ((), ())), preferred_element_type=F32
    )
    used, high, low, block, place_in = (table[p * 32 : (p + 1) * 32] for p in range(5))
    labels = jnp.where(used > 0.5, high * 32.0 + low, -1.0).astype(I32)
    for h in range(2):
        lab_ref[:, h, :] = labels[:, h * 128 : (h + 1) * 128]
    tok_ref[...] = jnp.where(used > 0.5, block * 64.0 + place_in, float(TOKS)).astype(I32)


def routing(token_ids, valid_counts):
    return pl.pallas_call(
        routing_kernel,
        grid_spec=pltpu.PrefetchScalarGridSpec(
            num_scalar_prefetch=1,
            grid=(1,),
            in_specs=[pl.BlockSpec((BLOCKS, BLOCK), lambda i, _: (0, 0))],
            out_specs=[
                pl.BlockSpec((32, CAP), lambda i, _: (0, 0)),
                pl.BlockSpec((32, 2, 128), lambda i, _: (0, 0, 0)),
            ],
            scratch_shapes=[pltpu.VMEM((160, TOKS), BF16), pltpu.VMEM((CAP, TOKS), BF16)],
        ),
        out_shape=(
            jax.ShapeDtypeStruct((32, CAP), I32),
            jax.ShapeDtypeStruct((32, 2, 128), I32),
        ),
        name="routing",
    )(valid_counts, token_ids.reshape(BLOCKS, BLOCK))


ROW_AXES = ("z", "y", "x")
FIRST = ("x", "z", "y")
SECOND = ("y", "x", "z")
STEPS = (2, 1, 3, 0)


def quarter(ref, q):
    return ref.at[pl.ds(pl.multiple_of(q * QROWS, 16), QROWS)]


ROWS = 512
SUB = 64
PLANE = TOKS + 8
STAGE = CAP + 8


def row_grads(g, v, gain):
    x = v.astype(F32)
    cen = x - jnp.mean(x, axis=1, keepdims=True)
    inv = lax.rsqrt(jnp.mean(cen * cen, axis=1, keepdims=True) + 1e-12)
    scaled = gain * g.astype(F32)
    first = jnp.mean(scaled, axis=1, keepdims=True)
    second = jnp.mean(scaled * cen, axis=1, keepdims=True) * inv
    return inv * (scaled - first - cen * (inv * second))


def table_kernel(
    tok, lab, g_hbm, v_hbm, gain_ref, out,
    gbuf, vbuf, rows, stage, box, inbox, inlab, tab, got2a, got2, u0, u1, ub0, ub1, got3, f,
    load, s1, r1, sl, rl, own1, s2a, r2a, s2, r2, s3, r3, s4, r4,
):
    x, z, y, c = place()
    barrier = pltpu.get_barrier_semaphore()
    hops = [(a, d, dc) for a in ROW_AXES for d in (1, 2, 3) for dc in (0, 1)] + [("x", 0, 1)]
    for a, d, dc in hops:
        pl.semaphore_signal(barrier, 1, device_id=shifted(a, d, dc), device_id_type=MESH)
    for e in range(4):
        pl.semaphore_signal(barrier, 1, device_id=device(z, e, y, c), device_id_type=MESH)

    def remote(src, dst, send, recv, to):
        return pltpu.make_async_remote_copy(
            src_ref=src, dst_ref=dst, send_sem=send, recv_sem=recv, device_id=to, device_id_type=MESH
        )

    def owner_of(ch, r):
        return ((z if ch == 1 else y) + r) % 4

    def loads(i, slot):
        at = pl.ds(i * ROWS, ROWS)
        return (
            pltpu.make_async_copy(g_hbm.at[at], gbuf.at[slot], load.at[0, slot]),
            pltpu.make_async_copy(v_hbm.at[at], vbuf.at[slot], load.at[1, slot]),
        )

    for copy in loads(0, 0):
        copy.start()
    for j in range(6):
        rows[pl.ds(j * PLANE + TOKS, 8), :] = jnp.zeros((8, 128), F32)
    gain = gain_ref[...].reshape(1, 768)

    def grads(i, carry):
        slot = i % 2

        @pl.when(i + 1 < TOKS // ROWS)
        def _():
            for copy in loads(i + 1, 1 - slot):
                copy.start()

        for copy in loads(i, slot):
            copy.wait()

        def sub_block(k, carry):
            at = pl.ds(pl.multiple_of(k * SUB, SUB), SUB)
            dx = row_grads(gbuf[slot, at, :], vbuf[slot, at, :], gain)
            for j in range(6):
                to = pl.multiple_of(j * PLANE + i * ROWS + k * SUB, 8)
                rows[pl.ds(to, SUB), :] = dx[:, j * 128 : (j + 1) * 128]
            return carry

        lax.fori_loop(0, ROWS // SUB, sub_block, 0, unroll=2)
        return carry

    lax.fori_loop(0, TOKS // ROWS, grads, 0)
    pl.semaphore_wait(barrier, len(hops) + 4)

    def label_copy(ch, d, dc):
        q = (coordinate(ROW_AXES[ch]) + d) % 4
        cq = (c + dc) % 2
        src = lab.at[:, q, cq] if ch == 1 else lab.at[q, :, cq]
        k = d * 2 + dc
        if k == 0:
            return pltpu.make_async_copy(src, inlab.at[ch, 0], own1.at[ch])
        return remote(src, inlab.at[ch, k], sl.at[ch, k], rl.at[ch, k], shifted(ROW_AXES[ch], d, dc))

    routes = [(d, dc) for d in (2, 1, 3, 0) for dc in (0, 1)]
    labels = {}
    for d, dc in routes:
        for ch in range(3):
            labels[ch, d, dc] = label_copy(ch, d, dc)
            labels[ch, d, dc].start()

    blocks = [(ry, rz, dc) for ry in STEPS for rz in STEPS for dc in (0, 1)]

    def row_copy(ch, b):
        ry, rz, dc = blocks[b]
        r = rz if ch == 1 else ry
        d = (rz, ry, (z + rz - x + 4) % 4)[ch]
        k = d * 2 + dc
        return remote(
            box.at[ch, b], inbox.at[ch, r, k], s1.at[ch, r, k], r1.at[ch, r, k],
            shifted(ROW_AXES[ch], d, dc),
        )

    def on_rows(b, action):
        ry, rz, dc = blocks[b]
        if rz + dc:
            action(row_copy(0, b))
        if ry + dc:
            action(row_copy(1, b))
        if dc:
            action(row_copy(2, b))
        else:

            @pl.when((z + rz) % 4 != x)
            def _():
                action(row_copy(2, b))

    for b, (ry, rz, dc) in enumerate(blocks):
        w = (z + rz) % 4 * 8 + (y + ry) % 4 * 2 + (c + dc) % 2
        at = b % 2 * 6 * STAGE

        def gather(i, carry):
            for e in range(16):
                t = tok[w, i * 16 + e]
                stage[pl.ds(at + i * 16 + e, 6, stride=STAGE), :] = rows[pl.ds(t, 6, stride=PLANE), :]
            return carry

        lax.fori_loop(0, CAP // 16, gather, 0)
        for ch in range(3):
            block = jnp.concatenate(
                [stage[pl.ds(at + (ch * 2 + h) * STAGE, CAP), :].astype(BF16) for h in range(2)], axis=1
            )
            if ch == 0 and rz + dc == 0:
                inbox[0, ry, 0] = block
            elif ch == 1 and ry + dc == 0:
                inbox[1, rz, 0] = block
            else:
                box[ch, b] = block
                if ch == 2 and dc == 0:

                    @pl.when((z + rz) % 4 == x)
                    def _():
                        inbox[2, ry, 0] = box[2, b]

        if b > 0:
            on_rows(b - 1, lambda copy: copy.start())
    on_rows(31, lambda copy: copy.start())

    def arrived(ch, r, d, dc):
        if d + dc:
            k = d * 2 + dc
            remote(
                box.at[ch, 0], inbox.at[ch, r, k], s1.at[ch, r, k], r1.at[ch, r, k],
                shifted(ROW_AXES[ch], d, dc),
            ).wait_recv()

    twos = {}
    for d, dc in routes:
        for ch in range(3):
            if d + dc:
                labels[ch, d, dc].wait_recv()
            else:
                labels[ch, d, dc].wait()
    order = [(ch, r) for r in (2, 1, 3) for ch in (0, 2)]
    order += [(1, 2), (0, 0), (1, 1), (1, 3), (2, 0), (1, 0)]
    for ch, r in order:
        if True:
            for d, dc in routes:
                arrived(ch, r, d, dc)
            w = owner_of(ch, r)

            def part(m, carry):
                ids = lax.broadcasted_iota(I32, (QROWS, 128), 0) + m * QROWS
                total = None
                for k in range(8):
                    picks = jnp.concatenate(
                        [
                            jnp.where(ids == inlab[ch, k, w, pl.ds(h, 1), :], 1.0, 0.0).astype(BF16)
                            for h in range(2)
                        ],
                        axis=1,
                    )
                    add = jnp.dot(picks, inbox[ch, r, k], preferred_element_type=F32)
                    total = add if total is None else total + add
                at = pl.ds(pl.multiple_of(m * QROWS, 16), QROWS)
                if ch > 0 and r == 0:
                    u1[ch - 1, at, :] = total
                else:
                    tab[ch, r, at, :] = total.astype(BF16)
                if ch == 0:

                    @pl.when(m == x)
                    def _():
                        u0[r] = total

                return carry

            lax.fori_loop(0, 4, part, 0)
            if ch == 0:
                for d in (2, 1, 3):
                    twos[0, r, d] = remote(
                        quarter(tab.at[0, r], (x + d) % 4), got2a.at[r, d - 1],
                        s2a.at[r, d - 1], r2a.at[r, d - 1], shifted("x", d),
                    )
                    twos[0, r, d].start()
            elif r > 0:
                twos[ch, r] = remote(
                    tab.at[ch, r], got2.at[ch - 1, r - 1],
                    s2.at[ch - 1, r - 1], r2.at[ch - 1, r - 1], shifted(FIRST[ch], r),
                )
                twos[ch, r].start()

    threes = {}
    for r in STEPS:
        for d in (2, 1, 3):
            twos[0, r, d].wait_recv()
        total = u0[r]
        for d in range(3):
            total += got2a[r, d].astype(F32)
        if r == 0:
            u0[0] = total
        else:
            ub0[r - 1] = total.astype(BF16)
            threes[0, r] = remote(
                ub0.at[r - 1], got3.at[0, r - 1], s3.at[0, r - 1], r3.at[0, r - 1], shifted("y", r)
            )
            threes[0, r].start()
    for ch in (1, 2):
        for r in (2, 1, 3):
            twos[ch, r].wait_recv()
        me = coordinate(SECOND[ch])
        for d in (2, 1, 3, 0):
            at = pl.ds(pl.multiple_of((me + d) % 4 * QROWS, 16), QROWS)
            total = u1[ch - 1, at, :]
            for e in range(3):
                total += got2[ch - 1, e, at, :].astype(F32)
            if d == 0:
                u1[ch - 1, at, :] = total
            else:
                ub1[ch - 1, d - 1] = total.astype(BF16)
                threes[ch, d] = remote(
                    ub1.at[ch - 1, d - 1], got3.at[ch, d - 1],
                    s3.at[ch, d - 1], r3.at[ch, d - 1], shifted(SECOND[ch], d),
                )
                threes[ch, d].start()

    fours = []
    for ch in range(3):
        for d in (2, 1, 3):
            threes[ch, d].wait_recv()
        if ch == 0:
            total = u0[0]
        else:
            me = coordinate(SECOND[ch])
            total = u1[ch - 1, pl.ds(pl.multiple_of(me * QROWS, 16), QROWS), :]
        for d in range(3):
            total += got3[ch, d].astype(F32)
        f[ch] = total.astype(BF16)
        if ch < 2:
            mine = out.at[pl.ds(pl.multiple_of(x * QROWS, 16), QROWS), pl.ds(ch * 256, 256)]
            mine[...] = f[ch]
            for d in (2, 1, 3):
                copy = remote(f.at[ch], mine, s4.at[ch, d], r4.at[ch, d], shifted("x", d))
                copy.start()
                fours.append(copy)

    mine = out.at[pl.ds(pl.multiple_of(z * QROWS, 16), QROWS), pl.ds(512, 256)]

    def last(e):
        return remote(f.at[2], mine, s4.at[2, e], r4.at[2, z], device((x + e) % 4, x, y, c))

    @pl.when(x == z)
    def _():
        mine[...] = f[2]

    @pl.when(x != z)
    def _():
        last(0).start()

    for e in (2, 1, 3):
        last(e).start()
    for q in range(4):

        @pl.when(jnp.logical_or(x != z, q != z))
        def _():
            remote(
                f.at[2], out.at[pl.ds(q * QROWS, QROWS), pl.ds(512, 256)],
                s4.at[2, 0], r4.at[2, q], device(x, z, y, c),
            ).wait_recv()

    for copy in fours:
        copy.wait()

    @pl.when(x != z)
    def _():
        last(0).wait_send()

    for e in (2, 1, 3):
        last(e).wait_send()
    for ch, d, dc in labels:
        if d + dc:
            labels[ch, d, dc].wait_send()
    for b in range(32):
        on_rows(b, lambda copy: copy.wait_send())
    for copy in list(twos.values()) + list(threes.values()):
        copy.wait_send()


def table_sums(tok, labels, grads, values, gain):
    any_space = pl.BlockSpec(memory_space=pl.ANY)
    dma = pltpu.SemaphoreType.DMA
    return pl.pallas_call(
        table_kernel,
        out_shape=jax.ShapeDtypeStruct((VOCAB_DEV, 768), BF16),
        in_specs=[
            pl.BlockSpec(memory_space=pltpu.SMEM),
            any_space,
            any_space,
            any_space,
            pl.BlockSpec(memory_space=pltpu.VMEM),
        ],
        out_specs=pl.BlockSpec(memory_space=pltpu.VMEM),
        scratch_shapes=[
            pltpu.VMEM((2, ROWS, 768), BF16),
            pltpu.VMEM((2, ROWS, 768), BF16),
            pltpu.VMEM((6 * PLANE, 128), F32),
            pltpu.VMEM((2 * 6 * STAGE, 128), F32),
            pltpu.VMEM((3, 32, CAP, 256), BF16),
            pltpu.VMEM((3, 4, 8, CAP, 256), BF16),
            pltpu.VMEM((3, 8, 4, 2, 128), I32),
            pltpu.VMEM((3, 4, VOCAB_DEV, 256), BF16),
            pltpu.VMEM((4, 3, QROWS, 256), BF16),
            pltpu.VMEM((2, 3, VOCAB_DEV, 256), BF16),
            pltpu.VMEM((4, QROWS, 256), F32),
            pltpu.VMEM((2, VOCAB_DEV, 256), F32),
            pltpu.VMEM((3, QROWS, 256), BF16),
            pltpu.VMEM((2, 3, QROWS, 256), BF16),
            pltpu.VMEM((3, 3, QROWS, 256), BF16),
            pltpu.VMEM((3, QROWS, 256), BF16),
            dma((2, 2)),
            dma((3, 4, 8)),
            dma((3, 4, 8)),
            dma((3, 8)),
            dma((3, 8)),
            dma((3,)),
            dma((4, 3)),
            dma((4, 3)),
            dma((2, 3)),
            dma((2, 3)),
            dma((3, 3)),
            dma((3, 3)),
            dma((3, 4)),
            dma((3, 4)),
        ],
        compiler_params=pltpu.CompilerParams(
            collective_id=0, has_side_effects=True, vmem_limit_bytes=62 << 20
        ),
        name="table_sums",
    )(tok, labels.reshape(4, 4, 2, 2, 128), grads, values, gain)


def per_device(token_ids, valid_counts, grad_output, pre_norm, norm_gain):
    tok, labels = routing(token_ids, valid_counts)
    return table_sums(tok, labels, grad_output, pre_norm, norm_gain).astype(F32)


def solution(mesh):
    in_specs = (
        P(("dp", "vocab")),
        P(("dp", "vocab")),
        P(("dp", "vocab"), None),
        P(("dp", "vocab"), None),
        P(),
    )
    return jax.shard_map(
        per_device, mesh=mesh, in_specs=in_specs, out_specs=P("vocab", None), check_vma=False
    )
```

```python
import functools

import jax
import jax.numpy as jnp
from jax import lax
from jax.experimental import pallas as pl
from jax.experimental.pallas import tpu as pltpu
from jax.sharding import PartitionSpec as P

VOCAB_DEV = 960
BLOCK = 128
CAP = 256
QROWS = VOCAB_DEV // 4
HALF = VOCAB_DEV // 2
LOW, HIGH = 128, 112
MESH = pl.DeviceIdType.MESH
F32, BF16, I32 = jnp.float32, jnp.bfloat16, jnp.int32


def place():
    x = lax.axis_index("dp")
    v = lax.axis_index("vocab")
    return x, v // 8, (v // 2) % 4, v % 2


def device(x, z, y, c):
    return (x, z * 8 + y * 2 + c)


def shifted(axis, d, dc=0):
    x, z, y, c = place()
    c = (c + dc) % 2
    if axis == "x":
        return device((x + d) % 4, z, y, c)
    if axis == "y":
        return device(x, z, (y + d) % 4, c)
    return device(x, (z + d) % 4, y, c)


def coordinate(axis):
    x, z, y, _ = place()
    return {"x": x, "y": y, "z": z}[axis]


TOKS = 4096
BLOCKS = TOKS // BLOCK


def routing_kernel(counts, ids_ref, tok_ref, lab_ref, weights, slots):
    owner_row = lax.broadcasted_iota(I32, (32, BLOCK), 0)
    lane = lax.broadcasted_iota(I32, (1, BLOCK), 1)
    ids = ids_ref[...]
    owner = lax.shift_right_logical(ids * 34953, 25)
    within = ids - owner * VOCAB_DEV
    before = (
        lax.broadcasted_iota(I32, (BLOCK, BLOCK), 0) < lax.broadcasted_iota(I32, (BLOCK, BLOCK), 1)
    )
    before = jnp.where(before, 1.0, 0.0).astype(BF16)
    base = jnp.zeros((32, 1), F32)
    slot_row = lax.broadcasted_iota(I32, (CAP, BLOCK), 0)
    for b in range(BLOCKS):
        mark = owner_row == owner[b : b + 1]
        ones = jnp.where(mark, 1.0, 0.0)
        ahead = jnp.dot(ones.astype(BF16), before, preferred_element_type=F32)
        rank = jnp.sum(jnp.where(mark, ahead + base, 0.0), axis=0, keepdims=True).astype(I32)
        base = base + jnp.sum(ones, axis=1, keepdims=True)
        live = lane < counts[b]
        mark = jnp.logical_and(mark, live)
        off = within[b : b + 1]
        at = pl.ds(b * BLOCK, BLOCK)
        for p, value in enumerate(
            (
                jnp.ones((1, BLOCK), F32),
                lax.shift_right_logical(off, 5).astype(F32),
                (off & 31).astype(F32),
                (b * 2 + lax.shift_right_logical(lane, 6)).astype(F32),
                (lane & 63).astype(F32),
            )
        ):
            weights[pl.ds(p * 32, 32), at] = jnp.where(mark, value, 0.0).astype(BF16)
        slots[:, at] = jnp.where(slot_row == rank, 1.0, 0.0).astype(BF16)
    table = lax.dot_general(
        weights[...], slots[...], (((1,), (1,)), ((), ())), preferred_element_type=F32
    )
    used, high, low, block, place_in = (table[p * 32 : (p + 1) * 32] for p in range(5))
    labels = jnp.where(used > 0.5, high * 32.0 + low, -1.0).astype(I32)
    for h in range(2):
        lab_ref[:, h, :] = labels[:, h * 128 : (h + 1) * 128]
    tok_ref[...] = jnp.where(used > 0.5, block * 64.0 + place_in, float(TOKS)).astype(I32)


def routing(token_ids, valid_counts):
    return pl.pallas_call(
        routing_kernel,
        grid_spec=pltpu.PrefetchScalarGridSpec(
            num_scalar_prefetch=1,
            grid=(1,),
            in_specs=[pl.BlockSpec((BLOCKS, BLOCK), lambda i, _: (0, 0))],
            out_specs=[
                pl.BlockSpec((32, CAP), lambda i, _: (0, 0)),
                pl.BlockSpec((32, 2, 128), lambda i, _: (0, 0, 0)),
            ],
            scratch_shapes=[pltpu.VMEM((160, TOKS), BF16), pltpu.VMEM((CAP, TOKS), BF16)],
        ),
        out_shape=(
            jax.ShapeDtypeStruct((32, CAP), I32),
            jax.ShapeDtypeStruct((32, 2, 128), I32),
        ),
        name="routing",
    )(valid_counts, token_ids.reshape(BLOCKS, BLOCK))


ROW_AXES = ("z", "y", "x")
FIRST = ("x", "z", "y")
SECOND = ("y", "x", "z")
STEPS = (2, 1, 3, 0)


ROWS = 512
SUB = 128
PLANE = TOKS + 8
STAGE = CAP + 8


def row_grads(g, v, gain):
    x = v.astype(F32)
    cen = x - jnp.mean(x, axis=1, keepdims=True)
    inv = lax.rsqrt(jnp.mean(cen * cen, axis=1, keepdims=True) + 1e-12)
    scaled = gain * g.astype(F32)
    first = jnp.mean(scaled, axis=1, keepdims=True)
    second = jnp.mean(scaled * cen, axis=1, keepdims=True) * inv
    return inv * (scaled - first - cen * (inv * second))


def table_kernel(
    tok, lab, g_hbm, v_hbm, gain_ref, out,
    rows, stage, box, inbox, inlab, tab, got2a, got2, via0, via1, via2, mid0, mid1, mid2, u0, u1, ub0, ub1, got3, f,
    load, s1, r1, sl, rl, own1, s2a, r2a, s2, r2, s3, r3, s4, r4,
):
    x, z, y, c = place()
    barrier = pltpu.get_barrier_semaphore()
    hops = [(a, d, dc) for a in ROW_AXES for d in (1, 2, 3) for dc in (0, 1)] + [("x", 0, 1)]
    for a, d, dc in hops:
        pl.semaphore_signal(barrier, 1, device_id=shifted(a, d, dc), device_id_type=MESH)
    for e in range(4):
        pl.semaphore_signal(barrier, 1, device_id=device(z, e, y, c), device_id_type=MESH)

    def remote(src, dst, send, recv, to):
        return pltpu.make_async_remote_copy(
            src_ref=src, dst_ref=dst, send_sem=send, recv_sem=recv, device_id=to, device_id_type=MESH
        )

    def owner_of(ch, r):
        return ((z if ch == 1 else y) + r) % 4

    def loads(i):
        at = pl.ds(i * 2, 2)
        return [
            pltpu.make_async_copy(
                src.at[at, :, pl.ds(ch * 256, 256)],
                box.at[ch, pl.ds(half * 16 + i * 2, 2)],
                load.at[i, half, ch],
            )
            for half, src in enumerate((g_hbm, v_hbm))
            for ch in range(3)
        ]

    for i in range(TOKS // ROWS):
        for copy in loads(i):
            copy.start()
    for j in range(6):
        rows[pl.ds(j * PLANE + TOKS, 8), :] = jnp.zeros((8, 128), F32)
    gain = gain_ref[...].reshape(1, 768)

    def grads(i, carry):
        for copy in loads(i):
            copy.wait()

        def sub_block(k, carry):
            at = pl.ds(pl.multiple_of(k % (CAP // SUB) * SUB, SUB), SUB)
            block = i * 2 + k // (CAP // SUB)
            g, v = (
                jnp.concatenate([box[ch, half + block, at, :] for ch in range(3)], axis=1)
                for half in (0, 16)
            )
            dx = row_grads(g, v, gain)
            for j in range(6):
                to = pl.multiple_of(j * PLANE + i * ROWS + k * SUB, 8)
                rows[pl.ds(to, SUB), :] = dx[:, j * 128 : (j + 1) * 128]
            return carry

        lax.fori_loop(0, ROWS // SUB, sub_block, 0, unroll=2)
        return carry

    lax.fori_loop(0, TOKS // ROWS, grads, 0)
    pl.semaphore_wait(barrier, len(hops) + 4)

    def label_copy(ch, d, dc):
        q = (coordinate(ROW_AXES[ch]) + d) % 4
        cq = (c + dc) % 2
        src = lab.at[:, q, cq] if ch == 1 else lab.at[q, :, cq]
        k = d * 2 + dc
        if k == 0:
            return pltpu.make_async_copy(src, inlab.at[ch, 0], own1.at[ch])
        return remote(src, inlab.at[ch, k], sl.at[ch, k], rl.at[ch, k], shifted(ROW_AXES[ch], d, dc))

    routes = [(d, dc) for d in (2, 1, 3, 0) for dc in (0, 1)]
    labels = {}
    for d, dc in routes:
        for ch in range(3):
            labels[ch, d, dc] = label_copy(ch, d, dc)
            labels[ch, d, dc].start()

    blocks = [(ry, rz, dc) for ry in STEPS for rz in STEPS for dc in (0, 1)]

    def row_copy(ch, b):
        ry, rz, dc = blocks[b]
        r = rz if ch == 1 else ry
        d = (rz, ry, (z + rz - x + 4) % 4)[ch]
        k = d * 2 + dc
        return remote(
            box.at[ch, b], inbox.at[ch, r, k], s1.at[ch, r, k], r1.at[ch, r, k],
            shifted(ROW_AXES[ch], d, dc),
        )

    def on_rows(b, action):
        ry, rz, dc = blocks[b]
        if rz + dc:
            action(row_copy(0, b))
        if ry + dc:
            action(row_copy(1, b))
        if dc:
            action(row_copy(2, b))
        else:

            @pl.when((z + rz) % 4 != x)
            def _():
                action(row_copy(2, b))

    for b, (ry, rz, dc) in enumerate(blocks):
        w = (z + rz) % 4 * 8 + (y + ry) % 4 * 2 + (c + dc) % 2
        at = b % 2 * 6 * STAGE

        def gather(i, carry):
            for e in range(16):
                t = tok[w, i * 16 + e]
                stage[pl.ds(at + i * 16 + e, 6, stride=STAGE), :] = rows[pl.ds(t, 6, stride=PLANE), :]
            return carry

        lax.fori_loop(0, CAP // 16, gather, 0)
        for ch in range(3):
            block = jnp.concatenate(
                [stage[pl.ds(at + (ch * 2 + h) * STAGE, CAP), :].astype(BF16) for h in range(2)], axis=1
            )
            if ch == 0 and rz + dc == 0:
                inbox[0, ry, 0] = block
            elif ch == 1 and ry + dc == 0:
                inbox[1, rz, 0] = block
            else:
                box[ch, b] = block
                if ch == 2 and dc == 0:

                    @pl.when((z + rz) % 4 == x)
                    def _():
                        inbox[2, ry, 0] = box[2, b]

        if b > 0:
            on_rows(b - 1, lambda copy: copy.start())
    on_rows(31, lambda copy: copy.start())

    def arrived(ch, r, d, dc):
        if d + dc:
            k = d * 2 + dc
            remote(
                box.at[ch, 0], inbox.at[ch, r, k], s1.at[ch, r, k], r1.at[ch, r, k],
                shifted(ROW_AXES[ch], d, dc),
            ).wait_recv()

    twos = []

    def send2(ch, r, kind, src, dst):
        send, recv = (s2a.at[r, kind], r2a.at[r, kind]) if ch == 0 else (s2.at[ch - 1, kind], r2.at[ch - 1, kind])
        copy = remote(src, dst, send, recv, shifted(FIRST[ch], 3 if kind % 2 else 1))
        copy.start()
        twos.append(copy)
        return copy

    def rows_of(q, first, count):
        return pl.ds(pl.multiple_of(q * QROWS + first, 16), count)

    north, south = (x + 1) % 4, (x + 3) % 4
    relays = {}
    direct = {}

    def start_sums(ch, r):
        if ch == 0:
            t = tab.at[0, r]
            relays[0, r] = (
                send2(0, r, 0, t.at[rows_of((x + 2) % 4, 0, LOW)], via0.at[r]),
                send2(0, r, 1, t.at[rows_of((x + 2) % 4, LOW, HIGH)], via1.at[r]),
            )
            direct[0, r] = [
                send2(0, r, 2, t.at[rows_of(north, LOW, HIGH)], got2a.at[r, 0, pl.ds(LOW, HIGH)]),
                send2(0, r, 3, t.at[rows_of(south, 0, LOW)], got2a.at[r, 1, pl.ds(0, LOW)]),
            ]
        elif r == 2:
            relays[ch] = (
                send2(ch, r, 0, tab.at[ch, 2, pl.ds(0, HALF)], via2.at[ch - 1, 0]),
                send2(ch, r, 1, tab.at[ch, 2, pl.ds(HALF, HALF)], via2.at[ch - 1, 1]),
            )
            direct[ch] = []
        elif r == 1:
            direct[ch].append(
                send2(ch, r, 2, tab.at[ch, 1, pl.ds(HALF, HALF)], got2.at[ch - 1, 0, pl.ds(HALF, HALF)])
            )
        elif r == 3:
            direct[ch].append(
                send2(ch, r, 3, tab.at[ch, 3, pl.ds(0, HALF)], got2.at[ch - 1, 1, pl.ds(0, HALF)])
            )

    def relay(ch, r=None):
        if ch == 0:
            t = tab.at[0, r]
            relays[0, r][0].wait_recv()
            at = rows_of(north, 0, LOW)
            t[at, :] = (mid0[r] + via0[r].astype(F32)).astype(BF16)
            direct[0, r].append(send2(0, r, 4, t.at[at], got2a.at[r, 0, pl.ds(0, LOW)]))
            relays[0, r][1].wait_recv()
            at = rows_of(south, LOW, HIGH)
            t[at, :] = (mid1[r] + via1[r].astype(F32)).astype(BF16)
            direct[0, r].append(send2(0, r, 5, t.at[at], got2a.at[r, 1, pl.ds(LOW, HIGH)]))
        else:
            for side, (w, first) in enumerate(((1, 0), (3, HALF))):
                relays[ch][side].wait_recv()
                at = pl.ds(first, HALF)
                tab[ch, w, at, :] = (
                    mid2[ch - 1, side] + via2[ch - 1, side].astype(F32)
                ).astype(BF16)
                direct[ch].append(
                    send2(ch, w, 4 + side, tab.at[ch, w, at], got2.at[ch - 1, side, at])
                )

    for d, dc in routes:
        for ch in range(3):
            if d + dc:
                labels[ch, d, dc].wait_recv()
            else:
                labels[ch, d, dc].wait()

    def partial_table(ch, r):
        for d, dc in routes:
            arrived(ch, r, d, dc)
        w = owner_of(ch, r)

        def part(m, carry):
            ids = lax.broadcasted_iota(I32, (QROWS, 128), 0) + m * QROWS
            total = None
            for k in range(8):
                picks = jnp.concatenate(
                    [
                        jnp.where(ids == inlab[ch, k, w, pl.ds(h, 1), :], 1.0, 0.0).astype(BF16)
                        for h in range(2)
                    ],
                    axis=1,
                )
                add = jnp.dot(picks, inbox[ch, r, k], preferred_element_type=F32)
                total = add if total is None else total + add
            at = pl.ds(pl.multiple_of(m * QROWS, 16), QROWS)
            if ch > 0 and r == 0:
                u1[ch - 1, at, :] = total
            elif ch > 0 and r != 2:
                side, summed = (0, m < 2) if r == 1 else (1, m >= 2)

                @pl.when(summed)
                def _():
                    mid2[ch - 1, side, pl.ds(pl.multiple_of(m % 2 * QROWS, 16), QROWS), :] = total

                @pl.when(jnp.logical_not(summed))
                def _():
                    tab[ch, r, at, :] = total.astype(BF16)

            else:
                tab[ch, r, at, :] = total.astype(BF16)
            if ch == 0:

                @pl.when(m == x)
                def _():
                    u0[r] = total

                @pl.when(m == north)
                def _():
                    mid0[r] = total[:LOW]

                @pl.when(m == south)
                def _():
                    mid1[r] = total[LOW:]

            return carry

        lax.fori_loop(0, 4, part, 0)
        start_sums(ch, r)

    for r in (2, 1, 3):
        partial_table(0, r)
        partial_table(2, r)
    partial_table(1, 2)
    partial_table(0, 0)
    partial_table(1, 1)
    partial_table(1, 3)
    relay(0, 2)
    relay(0, 1)
    relay(2)
    partial_table(2, 0)
    partial_table(1, 0)
    relay(0, 3)
    relay(1)
    relay(0, 0)

    threes = {}
    for r in STEPS:
        for copy in direct[0, r]:
            copy.wait_recv()
        total = u0[r] + got2a[r, 0].astype(F32) + got2a[r, 1].astype(F32)
        if r == 0:
            u0[0] = total
        else:
            ub0[r - 1] = total.astype(BF16)
            threes[0, r] = remote(
                ub0.at[r - 1], got3.at[0, r - 1], s3.at[0, r - 1], r3.at[0, r - 1], shifted("y", r)
            )
            threes[0, r].start()
    for ch in (2, 1):
        for copy in direct[ch]:
            copy.wait_recv()
        me = coordinate(SECOND[ch])
        for d in (2, 1, 3, 0):
            at = pl.ds(pl.multiple_of((me + d) % 4 * QROWS, 16), QROWS)
            total = u1[ch - 1, at, :]
            for e in range(2):
                total += got2[ch - 1, e, at, :].astype(F32)
            if d == 0:
                u1[ch - 1, at, :] = total
            else:
                ub1[ch - 1, d - 1] = total.astype(BF16)
                threes[ch, d] = remote(
                    ub1.at[ch - 1, d - 1], got3.at[ch, d - 1],
                    s3.at[ch, d - 1], r3.at[ch, d - 1], shifted(SECOND[ch], d),
                )
                threes[ch, d].start()

    third = out.at[rows_of(z, 0, QROWS), pl.ds(512, 256)]

    def last(e):
        return remote(f.at[2], third, s4.at[2, e], r4.at[2, z], device((x + e) % 4, x, y, c))

    def last_chunk_starts():
        @pl.when(x == z)
        def _():
            third[...] = f[2]

        @pl.when(x != z)
        def _():
            last(0).start()

        for e in (2, 1, 3):
            last(e).start()

    fours = []
    fulls = {}
    for ch in (0, 2, 1):
        for d in (2, 1, 3):
            threes[ch, d].wait_recv()
        if ch == 0:
            total = u0[0]
        else:
            me = coordinate(SECOND[ch])
            total = u1[ch - 1, pl.ds(pl.multiple_of(me * QROWS, 16), QROWS), :]
        for d in range(3):
            total += got3[ch, d].astype(F32)
        f[ch] = total.astype(BF16)
        if ch < 2:
            mine = out.at[rows_of(x, 0, QROWS), pl.ds(ch * 256, 256)]
            mine[...] = f[ch]
            fulls[ch] = [
                remote(f.at[ch], mine, s4.at[ch, e], r4.at[ch, e], shifted("x", d))
                for e, d in enumerate((1, 3))
            ]
            for copy in fulls[ch]:
                copy.start()
        else:
            last_chunk_starts()
    for ch in (0, 1):
        for e, (q, first, count, d) in enumerate(((south, 0, LOW, 1), (north, LOW, HIGH, 3))):
            fulls[ch][e].wait_recv()
            piece = out.at[rows_of(q, first, count), pl.ds(ch * 256, 256)]
            copy = remote(piece, piece, s4.at[ch, 2 + e], r4.at[ch, 2 + e], shifted("x", d))
            copy.start()
            fours.append(copy)

    for q in range(4):

        @pl.when(jnp.logical_or(x != z, q != z))
        def _():
            remote(
                f.at[2], out.at[pl.ds(q * QROWS, QROWS), pl.ds(512, 256)],
                s4.at[2, 0], r4.at[2, q], device(x, z, y, c),
            ).wait_recv()

    for copy in fours:
        copy.wait()

    @pl.when(x != z)
    def _():
        last(0).wait_send()

    for e in (2, 1, 3):
        last(e).wait_send()
    for ch, d, dc in labels:
        if d + dc:
            labels[ch, d, dc].wait_send()
    for b in range(32):
        on_rows(b, lambda copy: copy.wait_send())
    for copy in twos + list(threes.values()) + fulls[0] + fulls[1]:
        copy.wait_send()


def table_sums(tok, labels, grads, values, gain):
    any_space = pl.BlockSpec(memory_space=pl.ANY)
    dma = pltpu.SemaphoreType.DMA
    return pl.pallas_call(
        table_kernel,
        out_shape=jax.ShapeDtypeStruct((VOCAB_DEV, 768), BF16),
        in_specs=[
            pl.BlockSpec(memory_space=pltpu.SMEM),
            any_space,
            any_space,
            any_space,
            pl.BlockSpec(memory_space=pltpu.VMEM),
        ],
        out_specs=pl.BlockSpec(memory_space=pltpu.VMEM),
        scratch_shapes=[
            pltpu.VMEM((6 * PLANE, 128), F32),
            pltpu.VMEM((2 * 6 * STAGE, 128), F32),
            pltpu.VMEM((3, 32, CAP, 256), BF16),
            pltpu.VMEM((3, 4, 8, CAP, 256), BF16),
            pltpu.VMEM((3, 8, 4, 2, 128), I32),
            pltpu.VMEM((3, 4, VOCAB_DEV, 256), BF16),
            pltpu.VMEM((4, 2, QROWS, 256), BF16),
            pltpu.VMEM((2, 2, VOCAB_DEV, 256), BF16),
            pltpu.VMEM((4, LOW, 256), BF16),
            pltpu.VMEM((4, HIGH, 256), BF16),
            pltpu.VMEM((2, 2, HALF, 256), BF16),
            pltpu.VMEM((4, LOW, 256), F32),
            pltpu.VMEM((4, HIGH, 256), F32),
            pltpu.VMEM((2, 2, HALF, 256), F32),
            pltpu.VMEM((4, QROWS, 256), F32),
            pltpu.VMEM((2, VOCAB_DEV, 256), F32),
            pltpu.VMEM((3, QROWS, 256), BF16),
            pltpu.VMEM((2, 3, QROWS, 256), BF16),
            pltpu.VMEM((3, 3, QROWS, 256), BF16),
            pltpu.VMEM((3, QROWS, 256), BF16),
            dma((TOKS // ROWS, 2, 3)),
            dma((3, 4, 8)),
            dma((3, 4, 8)),
            dma((3, 8)),
            dma((3, 8)),
            dma((3,)),
            dma((4, 6)),
            dma((4, 6)),
            dma((2, 6)),
            dma((2, 6)),
            dma((3, 3)),
            dma((3, 3)),
            dma((3, 4)),
            dma((3, 4)),
        ],
        compiler_params=pltpu.CompilerParams(
            collective_id=0, has_side_effects=True, vmem_limit_bytes=62 << 20
        ),
        name="table_sums",
    )(
        tok, labels.reshape(4, 4, 2, 2, 128), grads.reshape(16, CAP, 768), values.reshape(16, CAP, 768), gain
    )


def per_device(token_ids, valid_counts, grad_output, pre_norm, norm_gain):
    tok, labels = routing(token_ids, valid_counts)
    return table_sums(tok, labels, grad_output, pre_norm, norm_gain).astype(F32)


def solution(mesh):
    in_specs = (
        P(("dp", "vocab")),
        P(("dp", "vocab")),
        P(("dp", "vocab"), None),
        P(("dp", "vocab"), None),
        P(),
    )
    return jax.shard_map(
        per_device, mesh=mesh, in_specs=in_specs, out_specs=P("vocab", None), check_vma=False
    )
```

```python
import functools

import jax
import jax.numpy as jnp
from jax import lax
from jax.experimental import pallas as pl
from jax.experimental.pallas import tpu as pltpu
from jax.sharding import PartitionSpec as P

VOCAB_DEV = 960
BLOCK = 128
CAP = 256
QROWS = VOCAB_DEV // 4
HALF = VOCAB_DEV // 2
LOW, HIGH = 128, 112
MESH = pl.DeviceIdType.MESH
F32, BF16, I32 = jnp.float32, jnp.bfloat16, jnp.int32


def place():
    x = lax.axis_index("dp")
    v = lax.axis_index("vocab")
    return x, v // 8, (v // 2) % 4, v % 2


def device(x, z, y, c):
    return (x, z * 8 + y * 2 + c)


def shifted(axis, d, dc=0):
    x, z, y, c = place()
    c = (c + dc) % 2
    if axis == "x":
        return device((x + d) % 4, z, y, c)
    if axis == "y":
        return device(x, z, (y + d) % 4, c)
    return device(x, (z + d) % 4, y, c)


def coordinate(axis):
    x, z, y, _ = place()
    return {"x": x, "y": y, "z": z}[axis]


TOKS = 4096
BLOCKS = TOKS // BLOCK


def routing_kernel(counts, ids_ref, tok_ref, lab_ref, weights, slots):
    owner_row = lax.broadcasted_iota(I32, (32, BLOCK), 0)
    lane = lax.broadcasted_iota(I32, (1, BLOCK), 1)
    ids = ids_ref[...]
    owner = lax.shift_right_logical(ids * 34953, 25)
    within = ids - owner * VOCAB_DEV
    before = (
        lax.broadcasted_iota(I32, (BLOCK, BLOCK), 0) < lax.broadcasted_iota(I32, (BLOCK, BLOCK), 1)
    )
    before = jnp.where(before, 1.0, 0.0).astype(BF16)
    base = jnp.zeros((32, 1), F32)
    slot_row = lax.broadcasted_iota(I32, (CAP, BLOCK), 0)
    for b in range(BLOCKS):
        mark = owner_row == owner[b : b + 1]
        ones = jnp.where(mark, 1.0, 0.0)
        ahead = jnp.dot(ones.astype(BF16), before, preferred_element_type=F32)
        rank = jnp.sum(jnp.where(mark, ahead + base, 0.0), axis=0, keepdims=True).astype(I32)
        base = base + jnp.sum(ones, axis=1, keepdims=True)
        live = lane < counts[b]
        mark = jnp.logical_and(mark, live)
        off = within[b : b + 1]
        at = pl.ds(b * BLOCK, BLOCK)
        for p, value in enumerate(
            (
                jnp.ones((1, BLOCK), F32),
                lax.shift_right_logical(off, 5).astype(F32),
                (off & 31).astype(F32),
                (b * 2 + lax.shift_right_logical(lane, 6)).astype(F32),
                (lane & 63).astype(F32),
            )
        ):
            weights[pl.ds(p * 32, 32), at] = jnp.where(mark, value, 0.0).astype(BF16)
        slots[:, at] = jnp.where(slot_row == rank, 1.0, 0.0).astype(BF16)
    table = lax.dot_general(
        weights[...], slots[...], (((1,), (1,)), ((), ())), preferred_element_type=F32
    )
    used, high, low, block, place_in = (table[p * 32 : (p + 1) * 32] for p in range(5))
    toks = jnp.where(used > 0.5, block * 64.0 + place_in, float(TOKS)).astype(I32)
    labels = jnp.where(used > 0.5, high * 32.0 + low, -1.0).astype(I32)
    for h in range(2):
        lab_ref[:, h, :] = labels[:, h * 128 : (h + 1) * 128]
        tok_ref[:, h, :] = toks[:, h * 128 : (h + 1) * 128]


def routing(token_ids, valid_counts):
    return pl.pallas_call(
        routing_kernel,
        grid_spec=pltpu.PrefetchScalarGridSpec(
            num_scalar_prefetch=1,
            grid=(1,),
            in_specs=[pl.BlockSpec((BLOCKS, BLOCK), lambda i, _: (0, 0))],
            out_specs=[pl.BlockSpec((32, 2, 128), lambda i, _: (0, 0, 0))] * 2,
            scratch_shapes=[pltpu.VMEM((160, TOKS), BF16), pltpu.VMEM((CAP, TOKS), BF16)],
        ),
        out_shape=(jax.ShapeDtypeStruct((32, 2, 128), I32),) * 2,
        name="routing",
    )(valid_counts, token_ids.reshape(BLOCKS, BLOCK))


ROW_AXES = ("z", "y", "x")
FIRST = ("x", "z", "y")
SECOND = ("y", "x", "z")
STEPS = (2, 1, 3, 0)


ROWS = 512
SUB = 128
PLANE = TOKS + 8
STAGE = CAP + 8


def row_grads(g, v, gain):
    x = v.astype(F32)
    cen = x - jnp.mean(x, axis=1, keepdims=True)
    inv = lax.rsqrt(jnp.mean(cen * cen, axis=1, keepdims=True) + 1e-12)
    scaled = gain * g.astype(F32)
    first = jnp.mean(scaled, axis=1, keepdims=True)
    second = jnp.mean(scaled * cen, axis=1, keepdims=True) * inv
    return inv * (scaled - first - cen * (inv * second))


def table_kernel(
    tok_hbm, lab, g_hbm, v_hbm, gain_ref, out,
    tok, rows, stage, box, inbox, inlab, tab, got2a, got2, via0, via1, via2, mid0, mid1, mid2, u0, u1, ub0, ub1, got3, f,
    load, tok_sem, s1, r1, sl, rl, own1, s2a, r2a, s2, r2, s3, r3, s4, r4,
):
    x, z, y, c = place()
    barrier = pltpu.get_barrier_semaphore()
    hops = [(a, d, dc) for a in ROW_AXES for d in (1, 2, 3) for dc in (0, 1)] + [("x", 0, 1)]
    for a, d, dc in hops:
        pl.semaphore_signal(barrier, 1, device_id=shifted(a, d, dc), device_id_type=MESH)
    for e in range(4):
        pl.semaphore_signal(barrier, 1, device_id=device(z, e, y, c), device_id_type=MESH)

    def remote(src, dst, send, recv, to):
        return pltpu.make_async_remote_copy(
            src_ref=src, dst_ref=dst, send_sem=send, recv_sem=recv, device_id=to, device_id_type=MESH
        )

    def owner_of(ch, r):
        return ((z if ch == 1 else y) + r) % 4

    def loads(i):
        at = pl.ds(i * 2, 2)
        return [
            pltpu.make_async_copy(
                src.at[at, :, pl.ds(ch * 256, 256)],
                box.at[ch, pl.ds(half * 16 + i * 2, 2)],
                load.at[i, half, ch],
            )
            for half, src in enumerate((g_hbm, v_hbm))
            for ch in range(3)
        ]

    tok_copy = pltpu.make_async_copy(tok_hbm, tok, tok_sem.at[0])
    for i in range(TOKS // ROWS):
        for copy in loads(i):
            copy.start()
        if i == 0:
            tok_copy.start()
    for j in range(6):
        rows[pl.ds(j * PLANE + TOKS, 8), :] = jnp.zeros((8, 128), F32)
    gain = gain_ref[...].reshape(1, 768)

    def grads(i, carry):
        for copy in loads(i):
            copy.wait()

        def sub_block(k, carry):
            at = pl.ds(pl.multiple_of(k % (CAP // SUB) * SUB, SUB), SUB)
            block = i * 2 + k // (CAP // SUB)
            g, v = (
                jnp.concatenate([box[ch, half + block, at, :] for ch in range(3)], axis=1)
                for half in (0, 16)
            )
            dx = row_grads(g, v, gain)
            for j in range(6):
                to = pl.multiple_of(j * PLANE + i * ROWS + k * SUB, 8)
                rows[pl.ds(to, SUB), :] = dx[:, j * 128 : (j + 1) * 128]
            return carry

        lax.fori_loop(0, ROWS // SUB, sub_block, 0, unroll=2)
        return carry

    lax.fori_loop(0, TOKS // ROWS, grads, 0)
    tok_copy.wait()
    pl.semaphore_wait(barrier, len(hops) + 4)

    def label_copy(ch, d, dc):
        q = (coordinate(ROW_AXES[ch]) + d) % 4
        cq = (c + dc) % 2
        src = lab.at[:, q, cq] if ch == 1 else lab.at[q, :, cq]
        k = d * 2 + dc
        if k == 0:
            return pltpu.make_async_copy(src, inlab.at[ch, 0], own1.at[ch])
        return remote(src, inlab.at[ch, k], sl.at[ch, k], rl.at[ch, k], shifted(ROW_AXES[ch], d, dc))

    routes = [(d, dc) for d in (2, 1, 3, 0) for dc in (0, 1)]
    labels = {}
    for d, dc in routes:
        for ch in range(3):
            labels[ch, d, dc] = label_copy(ch, d, dc)
            labels[ch, d, dc].start()

    blocks = [(ry, rz, dc) for ry in STEPS for rz in STEPS for dc in (0, 1)]

    def row_copy(ch, b):
        ry, rz, dc = blocks[b]
        r = rz if ch == 1 else ry
        d = (rz, ry, (z + rz - x + 4) % 4)[ch]
        k = d * 2 + dc
        return remote(
            box.at[ch, b], inbox.at[ch, r, k], s1.at[ch, r, k], r1.at[ch, r, k],
            shifted(ROW_AXES[ch], d, dc),
        )

    def on_rows(b, action):
        ry, rz, dc = blocks[b]
        if rz + dc:
            action(row_copy(0, b))
        if ry + dc:
            action(row_copy(1, b))
        if dc:
            action(row_copy(2, b))
        else:

            @pl.when((z + rz) % 4 != x)
            def _():
                action(row_copy(2, b))

    for b, (ry, rz, dc) in enumerate(blocks):
        w = (z + rz) % 4 * 8 + (y + ry) % 4 * 2 + (c + dc) % 2
        at = b % 2 * 6 * STAGE

        def gather(i, carry):
            for e in range(16):
                t = tok[w * CAP + i * 16 + e]
                stage[pl.ds(at + i * 16 + e, 6, stride=STAGE), :] = rows[pl.ds(t, 6, stride=PLANE), :]
            return carry

        lax.fori_loop(0, CAP // 16, gather, 0)
        for ch in range(3):
            block = jnp.concatenate(
                [stage[pl.ds(at + (ch * 2 + h) * STAGE, CAP), :].astype(BF16) for h in range(2)], axis=1
            )
            if ch == 0 and rz + dc == 0:
                inbox[0, ry, 0] = block
            elif ch == 1 and ry + dc == 0:
                inbox[1, rz, 0] = block
            else:
                box[ch, b] = block
                if ch == 2 and dc == 0:

                    @pl.when((z + rz) % 4 == x)
                    def _():
                        inbox[2, ry, 0] = box[2, b]

        if b > 0:
            on_rows(b - 1, lambda copy: copy.start())
    on_rows(31, lambda copy: copy.start())

    def arrived(ch, r, d, dc):
        if d + dc:
            k = d * 2 + dc
            remote(
                box.at[ch, 0], inbox.at[ch, r, k], s1.at[ch, r, k], r1.at[ch, r, k],
                shifted(ROW_AXES[ch], d, dc),
            ).wait_recv()

    twos = []

    def send2(ch, r, kind, src, dst):
        send, recv = (s2a.at[r, kind], r2a.at[r, kind]) if ch == 0 else (s2.at[ch - 1, kind], r2.at[ch - 1, kind])
        copy = remote(src, dst, send, recv, shifted(FIRST[ch], 3 if kind % 2 else 1))
        copy.start()
        twos.append(copy)
        return copy

    def rows_of(q, first, count):
        return pl.ds(pl.multiple_of(q * QROWS + first, 16), count)

    north, south = (x + 1) % 4, (x + 3) % 4
    relays = {}
    direct = {}

    def start_sums(ch, r):
        if ch == 0:
            t = tab.at[0, r]
            relays[0, r] = (
                send2(0, r, 0, t.at[rows_of((x + 2) % 4, 0, LOW)], via0.at[r]),
                send2(0, r, 1, t.at[rows_of((x + 2) % 4, LOW, HIGH)], via1.at[r]),
            )
            direct[0, r] = [
                send2(0, r, 2, t.at[rows_of(north, LOW, HIGH)], got2a.at[r, 0, pl.ds(LOW, HIGH)]),
                send2(0, r, 3, t.at[rows_of(south, 0, LOW)], got2a.at[r, 1, pl.ds(0, LOW)]),
            ]
        elif r == 2:
            relays[ch] = (
                send2(ch, r, 0, tab.at[ch, 2, pl.ds(0, HALF)], via2.at[ch - 1, 0]),
                send2(ch, r, 1, tab.at[ch, 2, pl.ds(HALF, HALF)], via2.at[ch - 1, 1]),
            )
            direct[ch] = []
        elif r == 1:
            direct[ch].append(
                send2(ch, r, 2, tab.at[ch, 1, pl.ds(HALF, HALF)], got2.at[ch - 1, 0, pl.ds(HALF, HALF)])
            )
        elif r == 3:
            direct[ch].append(
                send2(ch, r, 3, tab.at[ch, 3, pl.ds(0, HALF)], got2.at[ch - 1, 1, pl.ds(0, HALF)])
            )

    def relay(ch, r=None):
        if ch == 0:
            t = tab.at[0, r]
            relays[0, r][0].wait_recv()
            at = rows_of(north, 0, LOW)
            t[at, :] = (mid0[r] + via0[r].astype(F32)).astype(BF16)
            direct[0, r].append(send2(0, r, 4, t.at[at], got2a.at[r, 0, pl.ds(0, LOW)]))
            relays[0, r][1].wait_recv()
            at = rows_of(south, LOW, HIGH)
            t[at, :] = (mid1[r] + via1[r].astype(F32)).astype(BF16)
            direct[0, r].append(send2(0, r, 5, t.at[at], got2a.at[r, 1, pl.ds(LOW, HIGH)]))
        else:
            for side, (w, first) in enumerate(((1, 0), (3, HALF))):
                relays[ch][side].wait_recv()
                at = pl.ds(first, HALF)
                tab[ch, w, at, :] = (
                    mid2[ch - 1, side] + via2[ch - 1, side].astype(F32)
                ).astype(BF16)
                direct[ch].append(
                    send2(ch, w, 4 + side, tab.at[ch, w, at], got2.at[ch - 1, side, at])
                )

    for d, dc in routes:
        for ch in range(3):
            if d + dc:
                labels[ch, d, dc].wait_recv()
            else:
                labels[ch, d, dc].wait()

    def partial_table(ch, r):
        for d, dc in routes:
            arrived(ch, r, d, dc)
        w = owner_of(ch, r)

        def part(m, carry):
            ids = lax.broadcasted_iota(I32, (QROWS, 128), 0) + m * QROWS
            total = None
            for k in range(8):
                picks = jnp.concatenate(
                    [
                        jnp.where(ids == inlab[ch, k, w, pl.ds(h, 1), :], 1.0, 0.0).astype(BF16)
                        for h in range(2)
                    ],
                    axis=1,
                )
                add = jnp.dot(picks, inbox[ch, r, k], preferred_element_type=F32)
                total = add if total is None else total + add
            at = pl.ds(pl.multiple_of(m * QROWS, 16), QROWS)
            if ch > 0 and r == 0:
                u1[ch - 1, at, :] = total
            elif ch > 0 and r != 2:
                side, summed = (0, m < 2) if r == 1 else (1, m >= 2)

                @pl.when(summed)
                def _():
                    mid2[ch - 1, side, pl.ds(pl.multiple_of(m % 2 * QROWS, 16), QROWS), :] = total

                @pl.when(jnp.logical_not(summed))
                def _():
                    tab[ch, r, at, :] = total.astype(BF16)

            else:
                tab[ch, r, at, :] = total.astype(BF16)
            if ch == 0:

                @pl.when(m == x)
                def _():
                    u0[r] = total

                @pl.when(m == north)
                def _():
                    mid0[r] = total[:LOW]

                @pl.when(m == south)
                def _():
                    mid1[r] = total[LOW:]

            return carry

        lax.fori_loop(0, 4, part, 0)
        start_sums(ch, r)

    for r in (2, 1, 3):
        partial_table(0, r)
        partial_table(2, r)
    partial_table(1, 2)
    partial_table(0, 0)
    partial_table(1, 1)
    partial_table(1, 3)
    relay(0, 2)
    relay(0, 1)
    relay(2)
    partial_table(2, 0)
    partial_table(1, 0)
    relay(0, 3)
    relay(1)
    relay(0, 0)

    threes = {}
    for r in STEPS:
        for copy in direct[0, r]:
            copy.wait_recv()
        total = u0[r] + got2a[r, 0].astype(F32) + got2a[r, 1].astype(F32)
        if r == 0:
            u0[0] = total
        else:
            ub0[r - 1] = total.astype(BF16)
            threes[0, r] = remote(
                ub0.at[r - 1], got3.at[0, r - 1], s3.at[0, r - 1], r3.at[0, r - 1], shifted("y", r)
            )
            threes[0, r].start()
    for ch in (2, 1):
        for copy in direct[ch]:
            copy.wait_recv()
        me = coordinate(SECOND[ch])
        for d in (2, 1, 3, 0):
            at = pl.ds(pl.multiple_of((me + d) % 4 * QROWS, 16), QROWS)
            total = u1[ch - 1, at, :]
            for e in range(2):
                total += got2[ch - 1, e, at, :].astype(F32)
            if d == 0:
                u1[ch - 1, at, :] = total
            else:
                ub1[ch - 1, d - 1] = total.astype(BF16)
                threes[ch, d] = remote(
                    ub1.at[ch - 1, d - 1], got3.at[ch, d - 1],
                    s3.at[ch, d - 1], r3.at[ch, d - 1], shifted(SECOND[ch], d),
                )
                threes[ch, d].start()

    third = out.at[rows_of(z, 0, QROWS), pl.ds(512, 256)]

    def last(e):
        return remote(f.at[2], third, s4.at[2, e], r4.at[2, z], device((x + e) % 4, x, y, c))

    def last_chunk_starts():
        @pl.when(x == z)
        def _():
            third[...] = f[2]

        @pl.when(x != z)
        def _():
            last(0).start()

        for e in (2, 1, 3):
            last(e).start()

    fours = []
    fulls = {}
    for ch in (0, 2, 1):
        for d in (2, 1, 3):
            threes[ch, d].wait_recv()
        if ch == 0:
            total = u0[0]
        else:
            me = coordinate(SECOND[ch])
            total = u1[ch - 1, pl.ds(pl.multiple_of(me * QROWS, 16), QROWS), :]
        for d in range(3):
            total += got3[ch, d].astype(F32)
        f[ch] = total.astype(BF16)
        if ch < 2:
            mine = out.at[rows_of(x, 0, QROWS), pl.ds(ch * 256, 256)]
            mine[...] = f[ch]
            fulls[ch] = [
                remote(f.at[ch], mine, s4.at[ch, e], r4.at[ch, e], shifted("x", d))
                for e, d in enumerate((1, 3))
            ]
            for copy in fulls[ch]:
                copy.start()
        else:
            last_chunk_starts()
    for ch in (0, 1):
        for e, (q, first, count, d) in enumerate(((south, 0, LOW, 1), (north, LOW, HIGH, 3))):
            fulls[ch][e].wait_recv()
            piece = out.at[rows_of(q, first, count), pl.ds(ch * 256, 256)]
            copy = remote(piece, piece, s4.at[ch, 2 + e], r4.at[ch, 2 + e], shifted("x", d))
            copy.start()
            fours.append(copy)

    for q in range(4):

        @pl.when(jnp.logical_or(x != z, q != z))
        def _():
            remote(
                f.at[2], out.at[pl.ds(q * QROWS, QROWS), pl.ds(512, 256)],
                s4.at[2, 0], r4.at[2, q], device(x, z, y, c),
            ).wait_recv()

    for copy in fours:
        copy.wait()

    @pl.when(x != z)
    def _():
        last(0).wait_send()

    for e in (2, 1, 3):
        last(e).wait_send()
    for ch, d, dc in labels:
        if d + dc:
            labels[ch, d, dc].wait_send()
    for b in range(32):
        on_rows(b, lambda copy: copy.wait_send())
    for copy in twos + list(threes.values()) + fulls[0] + fulls[1]:
        copy.wait_send()


def table_sums(tok, labels, grads, values, gain):
    any_space = pl.BlockSpec(memory_space=pl.ANY)
    dma = pltpu.SemaphoreType.DMA
    return pl.pallas_call(
        table_kernel,
        out_shape=jax.ShapeDtypeStruct((VOCAB_DEV, 768), BF16),
        in_specs=[
            any_space,
            any_space,
            any_space,
            any_space,
            pl.BlockSpec(memory_space=pltpu.VMEM),
        ],
        out_specs=pl.BlockSpec(memory_space=pltpu.VMEM),
        scratch_shapes=[
            pltpu.SMEM((32 * CAP,), I32),
            pltpu.VMEM((6 * PLANE, 128), F32),
            pltpu.VMEM((2 * 6 * STAGE, 128), F32),
            pltpu.VMEM((3, 32, CAP, 256), BF16),
            pltpu.VMEM((3, 4, 8, CAP, 256), BF16),
            pltpu.VMEM((3, 8, 4, 2, 128), I32),
            pltpu.VMEM((3, 4, VOCAB_DEV, 256), BF16),
            pltpu.VMEM((4, 2, QROWS, 256), BF16),
            pltpu.VMEM((2, 2, VOCAB_DEV, 256), BF16),
            pltpu.VMEM((4, LOW, 256), BF16),
            pltpu.VMEM((4, HIGH, 256), BF16),
            pltpu.VMEM((2, 2, HALF, 256), BF16),
            pltpu.VMEM((4, LOW, 256), F32),
            pltpu.VMEM((4, HIGH, 256), F32),
            pltpu.VMEM((2, 2, HALF, 256), F32),
            pltpu.VMEM((4, QROWS, 256), F32),
            pltpu.VMEM((2, VOCAB_DEV, 256), F32),
            pltpu.VMEM((3, QROWS, 256), BF16),
            pltpu.VMEM((2, 3, QROWS, 256), BF16),
            pltpu.VMEM((3, 3, QROWS, 256), BF16),
            pltpu.VMEM((3, QROWS, 256), BF16),
            dma((TOKS // ROWS, 2, 3)),
            dma((1,)),
            dma((3, 4, 8)),
            dma((3, 4, 8)),
            dma((3, 8)),
            dma((3, 8)),
            dma((3,)),
            dma((4, 6)),
            dma((4, 6)),
            dma((2, 6)),
            dma((2, 6)),
            dma((3, 3)),
            dma((3, 3)),
            dma((3, 4)),
            dma((3, 4)),
        ],
        compiler_params=pltpu.CompilerParams(
            collective_id=0, has_side_effects=True, vmem_limit_bytes=62 << 20
        ),
        name="table_sums",
    )(
        tok.reshape(32 * CAP), labels.reshape(4, 4, 2, 2, 128), grads.reshape(16, CAP, 768), values.reshape(16, CAP, 768), gain
    )


def per_device(token_ids, valid_counts, grad_output, pre_norm, norm_gain):
    tok, labels = routing(token_ids, valid_counts)
    return table_sums(tok, labels, grad_output, pre_norm, norm_gain).astype(F32)


def solution(mesh):
    in_specs = (
        P(("dp", "vocab")),
        P(("dp", "vocab")),
        P(("dp", "vocab"), None),
        P(("dp", "vocab"), None),
        P(),
    )
    return jax.shard_map(
        per_device, mesh=mesh, in_specs=in_specs, out_specs=P("vocab", None), check_vma=False
    )
```

```python
import functools

import jax
import jax.numpy as jnp
from jax import lax
from jax.experimental import pallas as pl
from jax.experimental.pallas import tpu as pltpu
from jax.sharding import PartitionSpec as P

VOCAB_DEV = 960
BLOCK = 128
CAP = 256
QROWS = VOCAB_DEV // 4
HALF = VOCAB_DEV // 2
LOW, HIGH = 128, 112
MESH = pl.DeviceIdType.MESH
F32, BF16, I32 = jnp.float32, jnp.bfloat16, jnp.int32


def place():
    x = lax.axis_index("dp")
    v = lax.axis_index("vocab")
    return x, v // 8, (v // 2) % 4, v % 2


def device(x, z, y, c):
    return (x, z * 8 + y * 2 + c)


def shifted(axis, d, dc=0):
    x, z, y, c = place()
    c = (c + dc) % 2
    if axis == "x":
        return device((x + d) % 4, z, y, c)
    if axis == "y":
        return device(x, z, (y + d) % 4, c)
    return device(x, (z + d) % 4, y, c)


def coordinate(axis):
    x, z, y, _ = place()
    return {"x": x, "y": y, "z": z}[axis]


TOKS = 4096
BLOCKS = TOKS // BLOCK


def routing_kernel(counts, ids_ref, tok_ref, lab_ref, weights, slots):
    owner_row = lax.broadcasted_iota(I32, (32, BLOCK), 0)
    lane = lax.broadcasted_iota(I32, (1, BLOCK), 1)
    ids = ids_ref[...]
    owner = lax.shift_right_logical(ids * 34953, 25)
    within = ids - owner * VOCAB_DEV
    before = (
        lax.broadcasted_iota(I32, (BLOCK, BLOCK), 0) < lax.broadcasted_iota(I32, (BLOCK, BLOCK), 1)
    )
    before = jnp.where(before, 1.0, 0.0).astype(BF16)
    base = jnp.zeros((32, 1), F32)
    slot_row = lax.broadcasted_iota(I32, (CAP, BLOCK), 0)
    for b in range(BLOCKS):
        mark = owner_row == owner[b : b + 1]
        ones = jnp.where(mark, 1.0, 0.0)
        ahead = jnp.dot(ones.astype(BF16), before, preferred_element_type=F32)
        rank = jnp.sum(jnp.where(mark, ahead + base, 0.0), axis=0, keepdims=True).astype(I32)
        base = base + jnp.sum(ones, axis=1, keepdims=True)
        live = lane < counts[b]
        mark = jnp.logical_and(mark, live)
        off = within[b : b + 1]
        at = pl.ds(b * BLOCK, BLOCK)
        for p, value in enumerate(
            (
                jnp.ones((1, BLOCK), F32),
                lax.shift_right_logical(off, 5).astype(F32),
                (off & 31).astype(F32),
                (b * 2 + lax.shift_right_logical(lane, 6)).astype(F32),
                (lane & 63).astype(F32),
            )
        ):
            weights[pl.ds(p * 32, 32), at] = jnp.where(mark, value, 0.0).astype(BF16)
        slots[:, at] = jnp.where(slot_row == rank, 1.0, 0.0).astype(BF16)
    table = lax.dot_general(
        weights[...], slots[...], (((1,), (1,)), ((), ())), preferred_element_type=F32
    )
    used, high, low, block, place_in = (table[p * 32 : (p + 1) * 32] for p in range(5))
    toks = jnp.where(used > 0.5, block * 64.0 + place_in, float(TOKS)).astype(I32)
    labels = jnp.where(used > 0.5, high * 32.0 + low, -1.0).astype(I32)
    for h in range(2):
        lab_ref[:, h, :] = labels[:, h * 128 : (h + 1) * 128]
        tok_ref[:, h, :] = toks[:, h * 128 : (h + 1) * 128]


def routing(token_ids, valid_counts):
    return pl.pallas_call(
        routing_kernel,
        in_specs=[pl.BlockSpec(memory_space=pltpu.SMEM), pl.BlockSpec(memory_space=pltpu.VMEM)],
        out_specs=[pl.BlockSpec(memory_space=pltpu.VMEM)] * 2,
        scratch_shapes=[pltpu.VMEM((160, TOKS), BF16), pltpu.VMEM((CAP, TOKS), BF16)],
        out_shape=(jax.ShapeDtypeStruct((32, 2, 128), I32),) * 2,
        name="routing",
    )(valid_counts, token_ids.reshape(BLOCKS, BLOCK))


ROW_AXES = ("z", "y", "x")
FIRST = ("x", "z", "y")
SECOND = ("y", "x", "z")
STEPS = (2, 1, 3, 0)


ROWS = 512
SUB = 128
PLANE = TOKS + 8
STAGE = CAP + 8


def row_grads(g, v, gain):
    x = v.astype(F32)
    cen = x - jnp.mean(x, axis=1, keepdims=True)
    inv = lax.rsqrt(jnp.mean(cen * cen, axis=1, keepdims=True) + 1e-12)
    scaled = gain * g.astype(F32)
    first = jnp.mean(scaled, axis=1, keepdims=True)
    second = jnp.mean(scaled * cen, axis=1, keepdims=True) * inv
    return inv * (scaled - first - cen * (inv * second))


def table_kernel(
    tok_hbm, lab, g_hbm, v_hbm, gain_ref, out,
    tok, rows, stage, box, inbox, inlab, tab, got2a, got2, via0, via1, via2, mid0, mid1, mid2, u0, u1, ub0, ub1, got3, f,
    load, tok_sem, s1, r1, sl, rl, own1, s2a, r2a, s2, r2, s3, r3, s4, r4,
):
    x, z, y, c = place()
    barrier = pltpu.get_barrier_semaphore()
    hops = [(a, d, dc) for a in ROW_AXES for d in (1, 2, 3) for dc in (0, 1)] + [("x", 0, 1)]
    for a, d, dc in hops:
        pl.semaphore_signal(barrier, 1, device_id=shifted(a, d, dc), device_id_type=MESH)
    for e in range(4):
        pl.semaphore_signal(barrier, 1, device_id=device(z, e, y, c), device_id_type=MESH)

    def remote(src, dst, send, recv, to):
        return pltpu.make_async_remote_copy(
            src_ref=src, dst_ref=dst, send_sem=send, recv_sem=recv, device_id=to, device_id_type=MESH
        )

    def owner_of(ch, r):
        return ((z if ch == 1 else y) + r) % 4

    def loads(i):
        at = pl.ds(i * 2, 2)
        return [
            pltpu.make_async_copy(
                src.at[at, :, pl.ds(ch * 256, 256)],
                box.at[ch, pl.ds(half * 16 + i * 2, 2)],
                load.at[i, half, ch],
            )
            for half, src in enumerate((g_hbm, v_hbm))
            for ch in range(3)
        ]

    tok_copy = pltpu.make_async_copy(tok_hbm, tok, tok_sem.at[0])
    for i in range(TOKS // ROWS):
        for copy in loads(i):
            copy.start()
        if i == 0:
            tok_copy.start()
    for j in range(6):
        rows[pl.ds(j * PLANE + TOKS, 8), :] = jnp.zeros((8, 128), F32)
    gain = gain_ref[...].reshape(1, 768)

    def grads(i, carry):
        for copy in loads(i):
            copy.wait()

        def sub_block(k, carry):
            at = pl.ds(pl.multiple_of(k % (CAP // SUB) * SUB, SUB), SUB)
            block = i * 2 + k // (CAP // SUB)
            g, v = (
                jnp.concatenate([box[ch, half + block, at, :] for ch in range(3)], axis=1)
                for half in (0, 16)
            )
            dx = row_grads(g, v, gain)
            for j in range(6):
                to = pl.multiple_of(j * PLANE + i * ROWS + k * SUB, 8)
                rows[pl.ds(to, SUB), :] = dx[:, j * 128 : (j + 1) * 128]
            return carry

        lax.fori_loop(0, ROWS // SUB, sub_block, 0, unroll=2)
        return carry

    lax.fori_loop(0, TOKS // ROWS, grads, 0)
    tok_copy.wait()
    pl.semaphore_wait(barrier, len(hops) + 4)

    def label_copy(ch, d, dc):
        q = (coordinate(ROW_AXES[ch]) + d) % 4
        cq = (c + dc) % 2
        src = lab.at[:, q, cq] if ch == 1 else lab.at[q, :, cq]
        k = d * 2 + dc
        if k == 0:
            return pltpu.make_async_copy(src, inlab.at[ch, 0], own1.at[ch])
        return remote(src, inlab.at[ch, k], sl.at[ch, k], rl.at[ch, k], shifted(ROW_AXES[ch], d, dc))

    routes = [(d, dc) for d in (2, 1, 3, 0) for dc in (0, 1)]
    labels = {}
    for d, dc in routes:
        for ch in range(3):
            labels[ch, d, dc] = label_copy(ch, d, dc)
            labels[ch, d, dc].start()

    blocks = [(ry, rz, dc) for ry in STEPS for rz in STEPS for dc in (0, 1)]

    def row_copy(ch, b):
        ry, rz, dc = blocks[b]
        r = rz if ch == 1 else ry
        d = (rz, ry, (z + rz - x + 4) % 4)[ch]
        k = d * 2 + dc
        return remote(
            box.at[ch, b], inbox.at[ch, r, k], s1.at[ch, r, k], r1.at[ch, r, k],
            shifted(ROW_AXES[ch], d, dc),
        )

    def on_rows(b, action):
        ry, rz, dc = blocks[b]
        if rz + dc:
            action(row_copy(0, b))
        if ry + dc:
            action(row_copy(1, b))
        if dc:
            action(row_copy(2, b))
        else:

            @pl.when((z + rz) % 4 != x)
            def _():
                action(row_copy(2, b))

    for b, (ry, rz, dc) in enumerate(blocks):
        w = (z + rz) % 4 * 8 + (y + ry) % 4 * 2 + (c + dc) % 2
        at = b % 2 * 6 * STAGE

        def gather(i, carry):
            for e in range(16):
                t = tok[w * CAP + i * 16 + e]
                stage[pl.ds(at + i * 16 + e, 6, stride=STAGE), :] = rows[pl.ds(t, 6, stride=PLANE), :]
            return carry

        lax.fori_loop(0, CAP // 16, gather, 0)
        for ch in range(3):
            block = jnp.concatenate(
                [stage[pl.ds(at + (ch * 2 + h) * STAGE, CAP), :].astype(BF16) for h in range(2)], axis=1
            )
            if ch == 0 and rz + dc == 0:
                inbox[0, ry, 0] = block
            elif ch == 1 and ry + dc == 0:
                inbox[1, rz, 0] = block
            else:
                box[ch, b] = block
                if ch == 2 and dc == 0:

                    @pl.when((z + rz) % 4 == x)
                    def _():
                        inbox[2, ry, 0] = box[2, b]

        if b > 0:
            on_rows(b - 1, lambda copy: copy.start())
    on_rows(31, lambda copy: copy.start())

    def arrived(ch, r, d, dc):
        if d + dc:
            k = d * 2 + dc
            remote(
                box.at[ch, 0], inbox.at[ch, r, k], s1.at[ch, r, k], r1.at[ch, r, k],
                shifted(ROW_AXES[ch], d, dc),
            ).wait_recv()

    twos = []

    def send2(ch, r, kind, src, dst):
        send, recv = (s2a.at[r, kind], r2a.at[r, kind]) if ch == 0 else (s2.at[ch - 1, kind], r2.at[ch - 1, kind])
        copy = remote(src, dst, send, recv, shifted(FIRST[ch], 3 if kind % 2 else 1))
        copy.start()
        twos.append(copy)
        return copy

    def rows_of(q, first, count):
        return pl.ds(pl.multiple_of(q * QROWS + first, 16), count)

    north, south = (x + 1) % 4, (x + 3) % 4
    relays = {}
    direct = {}

    def start_sums(ch, r):
        if ch == 0:
            t = tab.at[0, r]
            relays[0, r] = (
                send2(0, r, 0, t.at[rows_of((x + 2) % 4, 0, LOW)], via0.at[r]),
                send2(0, r, 1, t.at[rows_of((x + 2) % 4, LOW, HIGH)], via1.at[r]),
            )
            direct[0, r] = [
                send2(0, r, 2, t.at[rows_of(north, LOW, HIGH)], got2a.at[r, 0, pl.ds(LOW, HIGH)]),
                send2(0, r, 3, t.at[rows_of(south, 0, LOW)], got2a.at[r, 1, pl.ds(0, LOW)]),
            ]
        elif r == 2:
            relays[ch] = (
                send2(ch, r, 0, tab.at[ch, 2, pl.ds(0, HALF)], via2.at[ch - 1, 0]),
                send2(ch, r, 1, tab.at[ch, 2, pl.ds(HALF, HALF)], via2.at[ch - 1, 1]),
            )
            direct[ch] = []
        elif r == 1:
            direct[ch].append(
                send2(ch, r, 2, tab.at[ch, 1, pl.ds(HALF, HALF)], got2.at[ch - 1, 0, pl.ds(HALF, HALF)])
            )
        elif r == 3:
            direct[ch].append(
                send2(ch, r, 3, tab.at[ch, 3, pl.ds(0, HALF)], got2.at[ch - 1, 1, pl.ds(0, HALF)])
            )

    def relay(ch, r=None):
        if ch == 0:
            t = tab.at[0, r]
            relays[0, r][0].wait_recv()
            at = rows_of(north, 0, LOW)
            t[at, :] = (mid0[r] + via0[r].astype(F32)).astype(BF16)
            direct[0, r].append(send2(0, r, 4, t.at[at], got2a.at[r, 0, pl.ds(0, LOW)]))
            relays[0, r][1].wait_recv()
            at = rows_of(south, LOW, HIGH)
            t[at, :] = (mid1[r] + via1[r].astype(F32)).astype(BF16)
            direct[0, r].append(send2(0, r, 5, t.at[at], got2a.at[r, 1, pl.ds(LOW, HIGH)]))
        else:
            for side, (w, first) in enumerate(((1, 0), (3, HALF))):
                relays[ch][side].wait_recv()
                at = pl.ds(first, HALF)
                tab[ch, w, at, :] = (
                    mid2[ch - 1, side] + via2[ch - 1, side].astype(F32)
                ).astype(BF16)
                direct[ch].append(
                    send2(ch, w, 4 + side, tab.at[ch, w, at], got2.at[ch - 1, side, at])
                )

    for d, dc in routes:
        for ch in range(3):
            if d + dc:
                labels[ch, d, dc].wait_recv()
            else:
                labels[ch, d, dc].wait()

    def partial_table(ch, r):
        for d, dc in routes:
            arrived(ch, r, d, dc)
        w = owner_of(ch, r)

        def part(m, carry):
            ids = lax.broadcasted_iota(I32, (QROWS, 128), 0) + m * QROWS
            total = None
            for k in range(8):
                picks = jnp.concatenate(
                    [
                        jnp.where(ids == inlab[ch, k, w, pl.ds(h, 1), :], 1.0, 0.0).astype(BF16)
                        for h in range(2)
                    ],
                    axis=1,
                )
                add = jnp.dot(picks, inbox[ch, r, k], preferred_element_type=F32)
                total = add if total is None else total + add
            at = pl.ds(pl.multiple_of(m * QROWS, 16), QROWS)
            if ch > 0 and r == 0:
                u1[ch - 1, at, :] = total
            elif ch > 0 and r != 2:
                side, summed = (0, m < 2) if r == 1 else (1, m >= 2)

                @pl.when(summed)
                def _():
                    mid2[ch - 1, side, pl.ds(pl.multiple_of(m % 2 * QROWS, 16), QROWS), :] = total

                @pl.when(jnp.logical_not(summed))
                def _():
                    tab[ch, r, at, :] = total.astype(BF16)

            else:
                tab[ch, r, at, :] = total.astype(BF16)
            if ch == 0:

                @pl.when(m == x)
                def _():
                    u0[r] = total

                @pl.when(m == north)
                def _():
                    mid0[r] = total[:LOW]

                @pl.when(m == south)
                def _():
                    mid1[r] = total[LOW:]

            return carry

        lax.fori_loop(0, 4, part, 0)
        start_sums(ch, r)

    for r in (2, 1, 3):
        partial_table(0, r)
        partial_table(2, r)
    partial_table(1, 2)
    partial_table(0, 0)
    partial_table(1, 1)
    partial_table(1, 3)
    relay(0, 2)
    relay(0, 1)
    relay(2)
    partial_table(2, 0)
    partial_table(1, 0)
    relay(0, 3)
    relay(1)
    relay(0, 0)

    threes = {}
    for r in STEPS:
        for copy in direct[0, r]:
            copy.wait_recv()
        total = u0[r] + got2a[r, 0].astype(F32) + got2a[r, 1].astype(F32)
        if r == 0:
            u0[0] = total
        else:
            ub0[r - 1] = total.astype(BF16)
            threes[0, r] = remote(
                ub0.at[r - 1], got3.at[0, r - 1], s3.at[0, r - 1], r3.at[0, r - 1], shifted("y", r)
            )
            threes[0, r].start()
    for ch in (2, 1):
        for copy in direct[ch]:
            copy.wait_recv()
        me = coordinate(SECOND[ch])
        for d in (2, 1, 3, 0):
            at = pl.ds(pl.multiple_of((me + d) % 4 * QROWS, 16), QROWS)
            total = u1[ch - 1, at, :]
            for e in range(2):
                total += got2[ch - 1, e, at, :].astype(F32)
            if d == 0:
                u1[ch - 1, at, :] = total
            else:
                ub1[ch - 1, d - 1] = total.astype(BF16)
                threes[ch, d] = remote(
                    ub1.at[ch - 1, d - 1], got3.at[ch, d - 1],
                    s3.at[ch, d - 1], r3.at[ch, d - 1], shifted(SECOND[ch], d),
                )
                threes[ch, d].start()

    third = out.at[rows_of(z, 0, QROWS), pl.ds(512, 256)]

    def last(e):
        return remote(f.at[2], third, s4.at[2, e], r4.at[2, z], device((x + e) % 4, x, y, c))

    def last_chunk_starts():
        @pl.when(x == z)
        def _():
            third[...] = f[2]

        @pl.when(x != z)
        def _():
            last(0).start()

        for e in (2, 1, 3):
            last(e).start()

    fours = []
    fulls = {}
    for ch in (0, 1, 2):
        for d in (2, 1, 3):
            threes[ch, d].wait_recv()
        if ch == 0:
            total = u0[0]
        else:
            me = coordinate(SECOND[ch])
            total = u1[ch - 1, pl.ds(pl.multiple_of(me * QROWS, 16), QROWS), :]
        for d in range(3):
            total += got3[ch, d].astype(F32)
        f[ch] = total.astype(BF16)
        if ch < 2:
            mine = out.at[rows_of(x, 0, QROWS), pl.ds(ch * 256, 256)]
            mine[...] = f[ch]
            fulls[ch] = [
                remote(f.at[ch], mine, s4.at[ch, e], r4.at[ch, e], shifted("x", d))
                for e, d in enumerate((1, 3))
            ]
            for copy in fulls[ch]:
                copy.start()
        else:
            last_chunk_starts()
    for ch in (0, 1):
        for e, (q, first, count, d) in enumerate(((south, 0, LOW, 1), (north, LOW, HIGH, 3))):
            fulls[ch][e].wait_recv()
            piece = out.at[rows_of(q, first, count), pl.ds(ch * 256, 256)]
            copy = remote(piece, piece, s4.at[ch, 2 + e], r4.at[ch, 2 + e], shifted("x", d))
            copy.start()
            fours.append(copy)

    for q in range(4):

        @pl.when(jnp.logical_or(x != z, q != z))
        def _():
            remote(
                f.at[2], out.at[pl.ds(q * QROWS, QROWS), pl.ds(512, 256)],
                s4.at[2, 0], r4.at[2, q], device(x, z, y, c),
            ).wait_recv()

    for copy in fours:
        copy.wait()

    @pl.when(x != z)
    def _():
        last(0).wait_send()

    for e in (2, 1, 3):
        last(e).wait_send()
    for ch, d, dc in labels:
        if d + dc:
            labels[ch, d, dc].wait_send()
    for b in range(32):
        on_rows(b, lambda copy: copy.wait_send())
    for copy in twos + list(threes.values()) + fulls[0] + fulls[1]:
        copy.wait_send()


def table_sums(tok, labels, grads, values, gain):
    any_space = pl.BlockSpec(memory_space=pl.ANY)
    dma = pltpu.SemaphoreType.DMA
    return pl.pallas_call(
        table_kernel,
        out_shape=jax.ShapeDtypeStruct((VOCAB_DEV, 768), BF16),
        in_specs=[
            any_space,
            any_space,
            any_space,
            any_space,
            pl.BlockSpec(memory_space=pltpu.VMEM),
        ],
        out_specs=pl.BlockSpec(memory_space=pltpu.VMEM),
        scratch_shapes=[
            pltpu.SMEM((32 * CAP,), I32),
            pltpu.VMEM((6 * PLANE, 128), F32),
            pltpu.VMEM((2 * 6 * STAGE, 128), F32),
            pltpu.VMEM((3, 32, CAP, 256), BF16),
            pltpu.VMEM((3, 4, 8, CAP, 256), BF16),
            pltpu.VMEM((3, 8, 4, 2, 128), I32),
            pltpu.VMEM((3, 4, VOCAB_DEV, 256), BF16),
            pltpu.VMEM((4, 2, QROWS, 256), BF16),
            pltpu.VMEM((2, 2, VOCAB_DEV, 256), BF16),
            pltpu.VMEM((4, LOW, 256), BF16),
            pltpu.VMEM((4, HIGH, 256), BF16),
            pltpu.VMEM((2, 2, HALF, 256), BF16),
            pltpu.VMEM((4, LOW, 256), F32),
            pltpu.VMEM((4, HIGH, 256), F32),
            pltpu.VMEM((2, 2, HALF, 256), F32),
            pltpu.VMEM((4, QROWS, 256), F32),
            pltpu.VMEM((2, VOCAB_DEV, 256), F32),
            pltpu.VMEM((3, QROWS, 256), BF16),
            pltpu.VMEM((2, 3, QROWS, 256), BF16),
            pltpu.VMEM((3, 3, QROWS, 256), BF16),
            pltpu.VMEM((3, QROWS, 256), BF16),
            dma((TOKS // ROWS, 2, 3)),
            dma((1,)),
            dma((3, 4, 8)),
            dma((3, 4, 8)),
            dma((3, 8)),
            dma((3, 8)),
            dma((3,)),
            dma((4, 6)),
            dma((4, 6)),
            dma((2, 6)),
            dma((2, 6)),
            dma((3, 3)),
            dma((3, 3)),
            dma((3, 4)),
            dma((3, 4)),
        ],
        compiler_params=pltpu.CompilerParams(
            collective_id=0, has_side_effects=True, vmem_limit_bytes=62 << 20
        ),
        name="table_sums",
    )(
        tok.reshape(32 * CAP), labels.reshape(4, 4, 2, 2, 128), grads.reshape(16, CAP, 768), values.reshape(16, CAP, 768), gain
    )


def per_device(token_ids, valid_counts, grad_output, pre_norm, norm_gain):
    tok, labels = routing(token_ids, valid_counts)
    return table_sums(tok, labels, grad_output, pre_norm, norm_gain).astype(F32)


def solution(mesh):
    in_specs = (
        P(("dp", "vocab")),
        P(("dp", "vocab")),
        P(("dp", "vocab"), None),
        P(("dp", "vocab"), None),
        P(),
    )
    return jax.shard_map(
        per_device, mesh=mesh, in_specs=in_specs, out_specs=P("vocab", None), check_vma=False
    )
```
